32 devices in a mesh: vpair: 4 (over y, x), rank: 8 (over z, core).
Axes of the slice: x: 2, y: 2, z: 4, core: 2. Of those that a mesh axis runs over, the one named last changes fastest.
Arguments:
- amplitudes: bfloat16 [8, 1200, 1200], P(None, 'vpair', 'rank'), may hold values from -6 to 6
- factors: bfloat16 [1200, 8192], P('vpair', 'rank'), may hold values from -0.1875 to 0.1875
- kernel: bfloat16 [8192, 8192], P('vpair', 'rank'), may hold values from -0.875 to 0.875
- other_terms: float32 [8, 1200, 1200], P(None, 'vpair'), may hold values from -6 to 6
- virt_energy: float32 [1200], replicated, may hold values from 0.2 to 4
- pair_energy: float32 [8], replicated, may hold values from -3 to -0.5
Outputs:
- residual: float32 [8, 1200, 1200], P(None, 'vpair')
- update_rms: float32 [], replicated
The draws below stay inside these ranges and needn't reach their ends.
All inputs are finite; a program needn't handle non-finite values.
Results may differ from the reference program's by a relative error of at most 0.0035.
Values may be sent and summed in bfloat16 or wider, within the bound.
A program may use at most 192 MiB of HBM per device.

```python
import jax
import jax.numpy as jnp
from jax import lax

NVIR = 1200
NTHC = 8192
PAIRS = 8


def draw_virt_energy(key, part):
    jitter = jax.random.uniform(key, (NVIR,), jnp.float32)
    spread = (jnp.arange(NVIR, dtype=jnp.float32) + jitter) / NVIR
    return 0.2 + 3.8 * spread


def block_levels(rng, dims, split, smallest, largest):
    gain = 1.0
    for axis_at, parts in split:
        heights = jax.random.uniform(jax.random.fold_in(jax.random.fold_in(rng, 6), axis_at), (parts,), jnp.float32, smallest / len(split), largest / len(split))
        gain = gain * jnp.repeat(jnp.exp(heights), dims[axis_at] // parts).reshape((-1,) + (1,) * (len(dims) - 1 - axis_at))
    return gain


def centred(rng, shape, scale, limit, cuts=(), held_as=jnp.bfloat16):
    drawn = scale * jax.random.normal(rng, shape, jnp.float32)
    if cuts:
        drawn = drawn * block_levels(rng, shape, cuts, -0.22, 0.18)
    return jnp.clip(drawn, -limit, limit).astype(held_as)


def setup_inputs(seed: int = 0) -> dict:
    keys = jax.random.split(jax.random.key(seed), 7)
    amplitudes = centred(keys[0], (PAIRS, NVIR, NVIR), 1.0, 6.0, ((1, 4), (2, 8)))
    factors = centred(keys[1], (NVIR, NTHC), NVIR ** -0.5, 0.1875, ((0, 4), (1, 8)))
    kernel = centred(keys[2], (NTHC, NTHC), (NTHC * NTHC // (NVIR * NVIR)) ** -0.5, 0.875, ((0, 4), (1, 8)))
    other_terms = centred(keys[3], (PAIRS, NVIR, NVIR), 1.0, 6.0, ((1, 4),), jnp.float32)
    virt_energy = draw_virt_energy(jax.random.fold_in(keys[6], 71), 0)
    pair_energy = jnp.clip(jax.random.uniform(keys[5], (PAIRS,), jnp.float32, -3.0, -0.5), -3.0, -0.5)
    return dict(amplitudes=amplitudes, factors=factors, kernel=kernel, other_terms=other_terms, virt_energy=virt_energy, pair_energy=pair_energy)


epsilon = 1e-06

def reference(amplitudes, factors, kernel, other_terms, virt_energy, pair_energy):
    kernel_wide = kernel.astype(jnp.float32)

    def one_pair(operands):
        amplitude, other_block, pair_value = operands
        first_half = jnp.dot(amplitude, factors, preferred_element_type=jnp.float32).astype(jnp.bfloat16)
        coupled = jnp.dot(factors.T, first_half, preferred_element_type=jnp.float32)
        weighted = (kernel_wide * coupled).astype(jnp.bfloat16)
        back_half = jnp.dot(factors, weighted, preferred_element_type=jnp.float32).astype(jnp.bfloat16)
        ladder = jnp.dot(back_half, factors.T, preferred_element_type=jnp.float32)
        residual = other_block + ladder
        denominator = virt_energy[:, None] + virt_energy[None, :] - pair_value
        update = residual / denominator
        return (residual, jnp.sum(update * update))
    residual, squares = lax.map(one_pair, (amplitudes, other_terms, pair_energy))
    update_rms = jnp.sqrt(jnp.sum(squares) / (PAIRS * NVIR * NVIR) + epsilon)
    return (residual, update_rms)
```

```python
import functools

import jax
import jax.numpy as jnp
from jax import lax
from jax.experimental import pallas as pl
from jax.experimental.pallas import tpu as pltpu
from jax.sharding import PartitionSpec as P

epsilon = 1e-06


def shards(amplitudes, factors, kernel, other_terms, virt_energy, pair_energy):
    vpair_count = lax.axis_size("vpair")
    pair_count = amplitudes.shape[0]
    row_block = amplitudes.shape[1]
    col_block = amplitudes.shape[2]
    virt_count = row_block * vpair_count
    right_block = kernel.shape[1]
    factor_rows = lax.all_gather(factors, "rank", axis=1, tiled=True)
    factor_full = lax.all_gather(factor_rows, "vpair", axis=0, tiled=True)
    factor_cols = lax.dynamic_slice_in_dim(
        factor_full, lax.axis_index("rank") * right_block, right_block, 1
    )
    half_done = jnp.einsum(
        "ons,sh->onh",
        lax.all_gather(amplitudes, "rank", axis=2, tiled=True),
        factor_cols,
        preferred_element_type=jnp.float32,
    ).astype(jnp.bfloat16)
    kernel_sub = lax.all_to_all(kernel, "vpair", split_axis=1, concat_axis=0, tiled=True).astype(
        jnp.float32
    )
    coupled = jnp.einsum(
        "cp,icq->ipq",
        factor_full,
        lax.all_to_all(half_done, "vpair", split_axis=2, concat_axis=1, tiled=True),
        preferred_element_type=jnp.float32,
    )
    weighted = (kernel_sub[None] * coupled).astype(jnp.bfloat16)
    ladder_half = jnp.einsum(
        "ap,ipq->iaq", factor_full, weighted, preferred_element_type=jnp.float32
    ).astype(jnp.bfloat16)
    back_half = lax.all_to_all(ladder_half, "vpair", split_axis=1, concat_axis=2, tiled=True)
    partial_value = jnp.einsum(
        "iaq,bq->iab", back_half, factor_cols, preferred_element_type=jnp.float32
    )
    row_energy = lax.dynamic_slice_in_dim(
        virt_energy, lax.axis_index("vpair") * row_block, row_block, 0
    )
    ladder_share = lax.psum_scatter(partial_value, "rank", scatter_dimension=2, tiled=True)
    col_start = lax.axis_index("rank") * col_block
    own_terms = lax.dynamic_slice_in_dim(other_terms, col_start, col_block, 2)
    part_residual = own_terms + ladder_share
    col_energy = lax.dynamic_slice_in_dim(virt_energy, col_start, col_block, 0)
    denominator = row_energy[None, :, None] + col_energy[None, None, :] - pair_energy[:, None, None]
    update = part_residual / denominator
    squares = lax.psum(jnp.sum(update * update), ("vpair", "rank"))
    residual = lax.all_gather(part_residual, "rank", axis=2, tiled=True)
    update_rms = jnp.sqrt(squares / (pair_count * virt_count * virt_count) + epsilon)
    return (residual, update_rms)


MESH_IDS = pl.DeviceIdType.MESH


def middle_kernel(
    zs, own_ref, cols_ref, half_ref, kern_ref, out_ref, fall, hrecv, hturn, kturn, acc,
    loc_sem, hs, hr, fr, mr, zsend, xsend, msend, osem,
):
    v = lax.axis_index("vpair")
    r = lax.axis_index("rank")
    y, x = v // 2, v % 2
    z, core = r // 2, r % 2
    vx, vy, vd = y * 2 + 1 - x, (1 - y) * 2 + x, (1 - y) * 2 + 1 - x
    near = (vx, vy, vd)
    mate = z * 2 + 1 - core
    pairs, count, block, cols = hrecv.shape
    depth = own_ref.shape[1]
    rows = count * block
    group = 2
    groups = pairs // group
    tall = group * cols

    def rank_at(k, side):
        return ((z + k) % zs) * 2 + side

    barrier = pltpu.get_barrier_semaphore()
    peers = [(v, rank_at(k, core)) for k in range(1, zs)] + [(at, r) for at in near] + [(v, mate)]
    for peer in peers:
        pl.semaphore_signal(barrier, inc=1, device_id=peer, device_id_type=MESH_IDS)
    pl.semaphore_wait(barrier, len(peers))

    def remote(src, dst, send_sem, recv_sem, to):
        return pltpu.make_async_remote_copy(
            src_ref=src, dst_ref=dst, send_sem=send_sem, recv_sem=recv_sem,
            device_id=to, device_id_type=MESH_IDS,
        )

    def half_copy(i, j):
        at = pl.multiple_of(near[j] * cols, cols)
        return remote(
            half_ref.at[i, :, pl.ds(at, cols)], hrecv.at[i, v], hs.at[i, j], hr.at[i, v], (near[j], r)
        )

    def own_half(i):
        at = pl.multiple_of(v * cols, cols)
        return pltpu.make_async_copy(half_ref.at[i, :, pl.ds(at, cols)], hrecv.at[i, v], hr.at[i, v])

    def rows_copy(k):
        return remote(own_ref, fall.at[r, v], zsend.at[k], fr.at[r, v], (v, rank_at(k, core)))

    def side_copy(rr, at, k, j, to):
        return remote(fall.at[rr, at], fall.at[rr, at], xsend.at[k, j], fr.at[rr, at], (to, r))

    def mate_copy(k):
        rr = rank_at(k, core)
        return remote(fall.at[rr], fall.at[rr], msend.at[k], mr.at[rr], (v, mate))

    def shard_wait(rr, at):
        pltpu.make_async_copy(fall.at[rr, at], fall.at[rr, at], fr.at[rr, at]).wait()

    def block_wait(rr):
        pltpu.make_async_copy(fall.at[rr], fall.at[rr], mr.at[rr]).wait()

    def spread(k):
        rr = rank_at(k, core)
        shard_wait(rr, v)
        side_copy(rr, v, k, 0, vx).start()
        side_copy(rr, v, k, 1, vy).start()

    def relay_copy(k):
        rr = rank_at(k, core)
        odd = (rr // 2) % 2
        via = (y + odd * (1 - 2 * y)) * 2 + x + (1 - odd) * (1 - 2 * x)
        to = (y + (1 - odd) * (1 - 2 * y)) * 2 + x + odd * (1 - 2 * x)
        return side_copy(rr, via, k, 2, to)

    def relay(k):
        rr = rank_at(k, core)
        shard_wait(rr, vx)
        shard_wait(rr, vy)
        relay_copy(k).start()

    def finish(k):
        shard_wait(rank_at(k, core), vd)
        mate_copy(k).start()

    own_block = pltpu.make_async_copy(cols_ref, fall.at[r], loc_sem.at[0])
    mate_block = remote(cols_ref, fall.at[r], msend.at[0], mr.at[r], (v, mate))
    own_block.start()
    mate_block.start()
    for k in range(1, zs):
        rows_copy(k).start()

    @pl.loop(0, pairs)
    def _(i):
        for j in (0, 1, 2):
            half_copy(i, j).start()
        own_half(i).start()

    def turn_kernel(rr, slot):
        start = pl.multiple_of(rr * depth, depth)
        kturn[slot] = kern_ref[pl.ds(start, depth), :].T

    def compute(rr, slot, g):
        at = pl.multiple_of(g * tall, tall)
        shard = fall[rr].reshape(rows, depth)
        coupled = jnp.dot(hturn[pl.ds(at, tall), :], shard, preferred_element_type=jnp.float32)
        weight = kturn[slot].astype(jnp.float32)
        weighted = (coupled.reshape(group, cols, depth) * weight[None]).astype(jnp.bfloat16)
        return lax.dot_general(
            weighted.reshape(tall, depth), shard, (((1,), (1,)), ((), ())),
            preferred_element_type=jnp.float32,
        )

    turn_kernel(r, 0)
    turn_kernel(mate, 1)
    own_block.wait()
    block_wait(mate)

    @pl.loop(0, groups)
    def _(g):
        at = pl.multiple_of(g * tall, tall)
        for e in range(group):
            i = g * group + e
            for j in range(count):
                pltpu.make_async_copy(hrecv.at[i, j], hrecv.at[i, j], hr.at[i, j]).wait()
            hturn[pl.ds(at + e * cols, cols), :] = hrecv[i].reshape(rows, cols).T
        acc[pl.ds(at, tall), :] = compute(r, 0, g)
        acc[pl.ds(at, tall), :] += compute(mate, 1, g)

        @pl.when(g == 1)
        def _():
            spread(1)

    relay(1)
    spread(2)
    finish(1)

    @pl.loop(0, 2 * (zs - 1))
    def _(n):
        k = n // 2 + 1
        odd = n % 2
        rr = rank_at(k, core + odd - 2 * odd * core)

        @pl.when(odd == 1)
        def _():
            block_wait(rr)

        turn_kernel(rr, 0)

        @pl.loop(0, groups)
        def _(g):
            @pl.when(jnp.logical_and(k < zs - 1, jnp.logical_and(odd == 0, g == 1)))
            def _():
                relay(k + 1)

                @pl.when(k < zs - 2)
                def _():
                    spread(k + 2)

            @pl.when(jnp.logical_and(k < zs - 1, jnp.logical_and(odd == 1, g == 0)))
            def _():
                finish(k + 1)

            at = pl.multiple_of(g * tall, tall)
            acc[pl.ds(at, tall), :] += compute(rr, 0, g)

    def give(i):
        return pltpu.make_async_copy(hrecv.at[i], out_ref.at[i], osem.at[i])

    @pl.loop(0, pairs)
    def _(i):
        at = pl.multiple_of(i * cols, cols)
        hrecv[i] = acc[pl.ds(at, cols), :].astype(jnp.bfloat16).T.reshape(count, block, cols)
        give(i).start()

    mate_block.wait_send()
    for k in range(1, zs):
        rows_copy(k).wait_send()
        side_copy(r, v, k, 0, vx).wait_send()
        side_copy(r, v, k, 1, vy).wait_send()
        relay_copy(k).wait_send()
        mate_copy(k).wait_send()

    @pl.loop(0, pairs)
    def _(i):
        for j in (0, 1, 2):
            half_copy(i, j).wait_send()
        give(i).wait()


def front_kernel(zs, own_ref, amp_ref, cols_ref, amps_ref, mine_sem, cols_recv, amps_recv, cs, us, ds, ms, stage, hold):
    v = lax.axis_index("vpair")
    r = lax.axis_index("rank")
    y, x = v // 2, v % 2
    z, core = r // 2, r % 2
    near = (y * 2 + 1 - x, (1 - y) * 2 + x, (1 - y) * 2 + 1 - x)
    mate = z * 2 + 1 - core
    mesh_ids = pl.DeviceIdType.MESH
    has_up, has_down = z + 1 < zs, z >= 1
    up_to, down_to = ((z + 1) % zs) * 2 + core, ((z + zs - 1) % zs) * 2 + core

    barrier = pltpu.get_barrier_semaphore()
    peers = [(at, r) for at in near] + [(v, mate), (v, up_to), (v, down_to)]
    for peer in peers:
        pl.semaphore_signal(barrier, inc=1, device_id=peer, device_id_type=mesh_ids)
    pl.semaphore_wait(barrier, len(peers))

    def cols_copy(j, at, to):
        return pltpu.make_async_remote_copy(
            src_ref=own_ref, dst_ref=cols_ref.at[at], send_sem=cs.at[j], recv_sem=cols_recv.at[at],
            device_id=(to, r), device_id_type=mesh_ids,
        )

    def amps_copy(src, at, sem, to):
        return pltpu.make_async_remote_copy(
            src_ref=src, dst_ref=amps_ref.at[at], send_sem=sem, recv_sem=amps_recv.at[at],
            device_id=(v, to), device_id_type=mesh_ids,
        )

    def amps_wait(at):
        pltpu.make_async_copy(amps_ref.at[at], amps_ref.at[at], amps_recv.at[at]).wait()

    @pl.when(has_up)
    def _():
        amps_copy(amp_ref, r, us.at[0], up_to).start()

    @pl.when(has_down)
    def _():
        amps_copy(amp_ref, r, ds.at[0], down_to).start()

    for j in range(3):
        cols_copy(j, v, near[j]).start()
    amps_copy(amp_ref, r, ms.at[0, 0], mate).start()
    a = pltpu.make_async_copy(own_ref, stage, mine_sem.at[0])
    b = pltpu.make_async_copy(amp_ref, hold, mine_sem.at[1])
    a.start()
    b.start()
    a.wait()
    b.wait()
    c = pltpu.make_async_copy(stage, cols_ref.at[v], mine_sem.at[2])
    d = pltpu.make_async_copy(hold, amps_ref.at[r], mine_sem.at[3])
    c.start()
    d.start()
    c.wait()
    d.wait()

    for s in range(1, zs):
        low, high = ((z + zs - s) % zs) * 2 + core, ((z + s) % zs) * 2 + core

        @pl.when(z >= s)
        def _():
            amps_wait(low)
            amps_copy(amps_ref.at[low], low, ms.at[s, 0], mate).start()

            @pl.when(has_up)
            def _():
                amps_copy(amps_ref.at[low], low, us.at[s], up_to).start()

        @pl.when(z + s < zs)
        def _():
            amps_wait(high)
            amps_copy(amps_ref.at[high], high, ms.at[s, 1], mate).start()

            @pl.when(has_down)
            def _():
                amps_copy(amps_ref.at[high], high, ds.at[s], down_to).start()

    for at in near:
        pltpu.make_async_copy(cols_ref.at[at], cols_ref.at[at], cols_recv.at[at]).wait()
    for k in range(zs):
        amps_wait(k * 2 + 1 - core)
    for j in range(3):
        cols_copy(j, v, near[j]).wait_send()
    amps_copy(amp_ref, r, ms.at[0, 0], mate).wait_send()
    for s in range(zs):

        @pl.when(jnp.logical_and(z >= s, has_up))
        def _():
            amps_copy(amp_ref, r, us.at[s], up_to).wait_send()

        @pl.when(jnp.logical_and(z + s < zs, has_down))
        def _():
            amps_copy(amp_ref, r, ds.at[s], down_to).wait_send()

        if s:

            @pl.when(z >= s)
            def _():
                amps_copy(amp_ref, r, ms.at[s, 0], mate).wait_send()

            @pl.when(z + s < zs)
            def _():
                amps_copy(amp_ref, r, ms.at[s, 1], mate).wait_send()


def front_gather(factors_pad, amps_pad, vpair_count, rank_count):
    zs = rank_count // 2
    hbm = pl.BlockSpec(memory_space=pl.ANY)
    return pl.pallas_call(
        functools.partial(front_kernel, zs),
        out_shape=(
            jax.ShapeDtypeStruct((vpair_count, *factors_pad.shape), jnp.bfloat16),
            jax.ShapeDtypeStruct((rank_count, *amps_pad.shape), jnp.bfloat16),
        ),
        in_specs=[hbm, hbm],
        out_specs=(hbm, hbm),
        scratch_shapes=[
            pltpu.SemaphoreType.DMA((4,)),
            pltpu.SemaphoreType.DMA((vpair_count,)),
            pltpu.SemaphoreType.DMA((rank_count,)),
            pltpu.SemaphoreType.DMA((3,)),
            pltpu.SemaphoreType.DMA((zs,)),
            pltpu.SemaphoreType.DMA((zs,)),
            pltpu.SemaphoreType.DMA((zs, 2)),
            pltpu.VMEM(factors_pad.shape, jnp.bfloat16),
            pltpu.VMEM(amps_pad.shape, jnp.bfloat16),
        ],
        compiler_params=pltpu.CompilerParams(
            collective_id=1, has_side_effects=True, vmem_limit_bytes=60 * 1024 * 1024
        ),
        cost_estimate=pl.CostEstimate(flops=10**10, bytes_accessed=10**7, transcendentals=0),
    )(factors_pad, amps_pad)


def ladder_middle(factors_pad, cols_pad, half_done, kernel_sub, rank_count):
    count, block, depth = cols_pad.shape
    pairs = half_done.shape[0]
    cols = kernel_sub.shape[1]
    rows = count * block
    points = kernel_sub.shape[0]
    zs = rank_count // 2
    hbm = pl.BlockSpec(memory_space=pl.ANY)
    vmem = pl.BlockSpec(memory_space=pltpu.VMEM)
    dma = pltpu.SemaphoreType.DMA
    return pl.pallas_call(
        functools.partial(middle_kernel, zs),
        out_shape=jax.ShapeDtypeStruct((pairs, count, block, cols), jnp.bfloat16),
        in_specs=[hbm, hbm, hbm, vmem],
        out_specs=hbm,
        scratch_shapes=[
            pltpu.VMEM((rank_count, count, block, depth), jnp.bfloat16),
            pltpu.VMEM((pairs, count, block, cols), jnp.bfloat16),
            pltpu.VMEM((pairs * cols, rows), jnp.bfloat16),
            pltpu.VMEM((2, cols, depth), jnp.bfloat16),
            pltpu.VMEM((pairs * cols, rows), jnp.float32),
            dma((1,)),
            dma((pairs, 3)),
            dma((pairs, count)),
            dma((rank_count, count)),
            dma((rank_count,)),
            dma((zs,)),
            dma((zs, 3)),
            dma((zs,)),
            dma((pairs,)),
        ],
        compiler_params=pltpu.CompilerParams(
            collective_id=0, has_side_effects=True, vmem_limit_bytes=62 * 1024 * 1024
        ),
        cost_estimate=pl.CostEstimate(
            flops=4 * pairs * points * rows * cols, bytes_accessed=4 * points * rows, transcendentals=0
        ),
    )(factors_pad, cols_pad, half_done, kernel_sub)


def tail_kernel(
    back_ref, cols_ref, other_ref, rowen_ref, virt_ref, res_ref, sq_ref,
    rb, turned, part, msend, mrecv, zsend, outer, inner, fin, oth, sq, sqall,
    bs, br, ms, mr, zs_sem, outr, inr, fs, fr, osem, rsem, qs, qr,
):
    v = lax.axis_index("vpair")
    r = lax.axis_index("rank")
    y, x = v // 2, v % 2
    z, core = r // 2, r % 2
    near = (y * 2 + 1 - x, (1 - y) * 2 + x, (1 - y) * 2 + 1 - x)
    mate = z * 2 + 1 - core
    pairs, count, block, cols = rb.shape
    rows = part.shape[1]
    turns = pairs // 2
    at_end = jnp.logical_or(z == 0, z == 3)
    in_middle = jnp.logical_not(at_end)
    toward = jnp.where(z < 2, z + 1, z - 1)
    away = jnp.where(z == 1, 0, 3)
    toward_at = (v, toward * 2 + core)
    away_at = (v, away * 2 + core)
    mate_at = (v, mate)

    barrier = pltpu.get_barrier_semaphore()
    for peer in [(at, r) for at in near] + [mate_at, toward_at]:
        pl.semaphore_signal(barrier, inc=1, device_id=peer, device_id_type=MESH_IDS)

    @pl.when(in_middle)
    def _():
        pl.semaphore_signal(barrier, inc=1, device_id=away_at, device_id_type=MESH_IDS)
        pl.semaphore_wait(barrier, 6)

    @pl.when(at_end)
    def _():
        pl.semaphore_wait(barrier, 5)

    def remote(src, dst, send_sem, recv_sem, to):
        return pltpu.make_async_remote_copy(
            src_ref=src, dst_ref=dst, send_sem=send_sem, recv_sem=recv_sem,
            device_id=to, device_id_type=MESH_IDS,
        )

    def arrive(ref, sem):
        pltpu.make_async_copy(ref, ref, sem).wait()

    def back_copy(i, j):
        return remote(back_ref.at[i, near[j]], rb.at[i, v], bs.at[i, j], br.at[i, v], (near[j], r))

    def own_back(i):
        return pltpu.make_async_copy(back_ref.at[i, v], rb.at[i, v], br.at[i, v])

    @pl.loop(0, pairs)
    def _(i):
        for j in range(3):
            back_copy(i, j).start()
        own_back(i).start()

    def other_copy(p):
        return pltpu.make_async_copy(other_ref.at[:, p], oth.at[p % 4], osem.at[p % 4])

    def res_copy(p):
        return pltpu.make_async_copy(oth.at[p % 4], res_ref.at[:, p], rsem.at[p % 4])

    other_copy(0).start()
    other_copy(1).start()
    turned[...] = cols_ref[...].T

    def mate_copy(t):
        return remote(msend.at[t], mrecv.at[t], ms.at[t], mr.at[t], mate_at)

    def outer_copy(t):
        return remote(zsend.at[t], outer.at[t], zs_sem.at[t], outr.at[t], toward_at)

    def inner_copy(t):
        return remote(zsend.at[t], inner.at[t], zs_sem.at[t], inr.at[t], toward_at)

    def fin_copy(p, j, to):
        return remote(fin.at[p], fin.at[p], fs.at[p // 2, j], fr.at[p], to)

    def ladder(p):
        for j in range(count):
            arrive(rb.at[p, j], br.at[p, j])
        left = jnp.concatenate([rb[p, j] for j in range(count)], axis=1)
        return jnp.dot(left, turned[...], preferred_element_type=jnp.float32)[:rows]

    def step_a(t):
        msend[t] = ladder(2 * t + 1 - core).astype(jnp.bfloat16)
        mate_copy(t).start()
        part[t] = ladder(2 * t + core)

    def step_b(t):
        arrive(mrecv.at[t], mr.at[t])
        both = part[t] + mrecv[t].astype(jnp.float32)

        @pl.when(at_end)
        def _():
            zsend[t] = both.astype(jnp.bfloat16)
            outer_copy(t).start()

        @pl.when(in_middle)
        def _():
            part[t] = both

    def owner(t):
        return z == 1 + t % 2

    def step_c(t):
        @pl.when(in_middle)
        def _():
            arrive(outer.at[t], outr.at[t])
            three = part[t] + outer[t].astype(jnp.float32)

            @pl.when(owner(t))
            def _():
                part[t] = three

            @pl.when(jnp.logical_not(owner(t)))
            def _():
                zsend[t] = three.astype(jnp.bfloat16)
                inner_copy(t).start()

    def step_d(t):
        p = 2 * t + core

        @pl.when(jnp.logical_and(in_middle, owner(t)))
        def _():
            arrive(inner.at[t], inr.at[t])
            fin[p] = (part[t] + inner[t].astype(jnp.float32)).astype(jnp.bfloat16)
            fin_copy(p, 0, away_at).start()
            fin_copy(p, 1, toward_at).start()
            fin_copy(p, 2, mate_at).start()

        @pl.when(jnp.logical_and(in_middle, jnp.logical_not(owner(t))))
        def _():
            arrive(fin.at[p], fr.at[p])
            fin_copy(p, 0, away_at).start()
            fin_copy(p, 2, mate_at).start()

    def step_e(t):
        p = 2 * t + core

        @pl.when(at_end)
        def _():
            arrive(fin.at[p], fr.at[p])
            fin_copy(p, 2, mate_at).start()

    def settle(p):
        other_copy(p).wait()
        value = oth[p % 4] + fin[p].astype(jnp.float32)
        oth[p % 4] = value
        update = value / (rowen_ref[p] + virt_ref[...])
        sq[pl.ds(p, 1), :] = jnp.sum(update * update, axis=0, keepdims=True)
        res_copy(p).start()

    def step_f(t):
        arrive(fin.at[2 * t + 1 - core], fr.at[2 * t + 1 - core])

        @pl.when(t + 1 < turns)
        def _():
            for e in range(2):
                p = 2 * t + 2 + e

                @pl.when(t > 0)
                def _():
                    res_copy(p).wait()

                other_copy(p).start()

        for e in range(2):
            settle(2 * t + e)

    @pl.loop(0, turns + 5)
    def _(u):
        for lag, step in enumerate((step_a, step_b, step_c, step_d, step_e, step_f)):

            @pl.when(jnp.logical_and(u >= lag, u < turns + lag))
            def _():
                step(u - lag)

    sqall[v] = sq[...]
    for j in range(3):
        remote(sq, sqall.at[v], qs.at[j], qr.at[v], (near[j], r)).start()
    for at in near:
        arrive(sqall.at[at], qr.at[at])
    total = (sqall[0] + sqall[1]) + (sqall[2] + sqall[3])
    sq_ref[...] = jnp.sum(jnp.sum(total, axis=1, keepdims=True), axis=0, keepdims=True)

    for j in range(3):
        remote(sq, sqall.at[v], qs.at[j], qr.at[v], (near[j], r)).wait_send()

    @pl.loop(0, pairs)
    def _(i):
        for j in range(3):
            back_copy(i, j).wait_send()

    @pl.loop(0, turns)
    def _(t):
        p = 2 * t + core
        mate_copy(t).wait_send()
        fin_done = jnp.logical_and(in_middle, owner(t))

        @pl.when(jnp.logical_not(fin_done))
        def _():
            outer_copy(t).wait_send()

        @pl.when(in_middle)
        def _():
            fin_copy(p, 0, away_at).wait_send()

        @pl.when(fin_done)
        def _():
            fin_copy(p, 1, toward_at).wait_send()

        fin_copy(p, 2, mate_at).wait_send()

    for p in range(pairs - 4, pairs):
        res_copy(p).wait()


def ladder_tail(back, cols_flat, other_turned, row_energy, virt_energy):
    pairs, count, block, cols = back.shape
    rows = other_turned.shape[0]
    virt_count, depth = cols_flat.shape
    turns = pairs // 2
    hbm = pl.BlockSpec(memory_space=pl.ANY)
    vmem = pl.BlockSpec(memory_space=pltpu.VMEM)
    dma = pltpu.SemaphoreType.DMA
    bf16 = lambda *shape: pltpu.VMEM(shape, jnp.bfloat16)
    f32 = lambda *shape: pltpu.VMEM(shape, jnp.float32)
    return pl.pallas_call(
        tail_kernel,
        out_shape=(
            jax.ShapeDtypeStruct((rows, pairs, virt_count), jnp.float32),
            jax.ShapeDtypeStruct((1, 1), jnp.float32),
        ),
        in_specs=[hbm, vmem, hbm, vmem, vmem],
        out_specs=(hbm, vmem),
        scratch_shapes=[
            bf16(pairs, count, block, cols),
            bf16(depth, virt_count),
            f32(turns, rows, virt_count),
            bf16(turns, rows, virt_count),
            bf16(turns, rows, virt_count),
            bf16(turns, rows, virt_count),
            bf16(turns, rows, virt_count),
            bf16(turns, rows, virt_count),
            bf16(pairs, rows, virt_count),
            f32(4, rows, virt_count),
            f32(pairs, virt_count),
            f32(count, pairs, virt_count),
            dma((pairs, 3)),
            dma((pairs, count)),
            dma((turns,)),
            dma((turns,)),
            dma((turns,)),
            dma((turns,)),
            dma((turns,)),
            dma((turns, 3)),
            dma((pairs,)),
            dma((4,)),
            dma((4,)),
            dma((3,)),
            dma((count,)),
        ],
        compiler_params=pltpu.CompilerParams(
            collective_id=2, has_side_effects=True, vmem_limit_bytes=62 * 1024 * 1024
        ),
        cost_estimate=pl.CostEstimate(
            flops=2 * pairs * rows * virt_count * depth, bytes_accessed=8 * pairs * rows * virt_count,
            transcendentals=0,
        ),
    )(back, cols_flat, other_turned, row_energy, virt_energy)


def fast_shards(amplitudes, factors, kernel, other_terms, virt_energy, pair_energy):
    vpair_count = lax.axis_size("vpair")
    rank_count = lax.axis_size("rank")
    pair_count, row_block, _ = amplitudes.shape
    virt_count = row_block * vpair_count
    right_block = kernel.shape[1]
    block = -(-row_block // 16) * 16
    col_block = amplitudes.shape[2]
    deep = -(-col_block // 16) * 16
    kernel_sub = lax.all_to_all(kernel, "vpair", split_axis=1, concat_axis=0, tiled=True)
    factors_pad = jnp.pad(factors, ((0, block - row_block), (0, 0)))
    amps_pad = jnp.pad(
        amplitudes.transpose(2, 0, 1), ((0, deep - col_block), (0, 0), (0, block - row_block))
    ).reshape(deep, pair_count * block)
    cols_pad, amps = front_gather(factors_pad, amps_pad, vpair_count, rank_count)
    factor_cols = cols_pad[:, :row_block].reshape(virt_count, right_block)
    cols_deep = jnp.pad(
        factor_cols.reshape(rank_count, col_block, right_block), ((0, 0), (0, deep - col_block), (0, 0))
    ).reshape(rank_count * deep, right_block)
    half_done = jnp.einsum(
        "sm,sh->mh",
        amps.reshape(rank_count * deep, pair_count * block),
        cols_deep,
        preferred_element_type=jnp.float32,
    ).astype(jnp.bfloat16)
    half_done = half_done.reshape(pair_count, block, right_block)
    back = ladder_middle(factors_pad, cols_pad, half_done, kernel_sub, rank_count)
    row_energy = lax.dynamic_slice_in_dim(
        virt_energy, lax.axis_index("vpair") * row_block, row_block, 0
    )
    shifted = row_energy[None, :, None] - pair_energy[:, None, None]
    residual, squares = ladder_tail(
        back, factor_cols, other_terms.transpose(1, 0, 2), shifted, virt_energy[None, :]
    )
    update_rms = jnp.sqrt(squares[0, 0] / (pair_count * virt_count * virt_count) + epsilon)
    return (residual.transpose(1, 0, 2), update_rms)


def pick(amplitudes, factors, kernel, other_terms, virt_energy, pair_energy):
    vpair_count = lax.axis_size("vpair")
    rank_count = lax.axis_size("rank")
    fits = (
        vpair_count == 4
        and rank_count == 8
        and amplitudes.shape[0] == 8
        and kernel.shape[1] % (128 * vpair_count) == 0
    )
    body = fast_shards if fits else shards
    return body(amplitudes, factors, kernel, other_terms, virt_energy, pair_energy)


def solution(mesh):
    placed = (
        P(None, "vpair", "rank"),
        P("vpair", "rank"),
        P("vpair", "rank"),
        P(None, "vpair", None),
        P(),
        P(),
    )
    return jax.shard_map(
        pick, mesh=mesh, in_specs=placed, out_specs=(P(None, "vpair", None), P()), check_vma=False
    )
```

```python
import functools

import jax
import jax.numpy as jnp
from jax import lax
from jax.experimental import pallas as pl
from jax.experimental.pallas import tpu as pltpu
from jax.sharding import PartitionSpec as P

epsilon = 1e-06


def shards(amplitudes, factors, kernel, other_terms, virt_energy, pair_energy):
    vpair_count = lax.axis_size("vpair")
    pair_count = amplitudes.shape[0]
    row_block = amplitudes.shape[1]
    col_block = amplitudes.shape[2]
    virt_count = row_block * vpair_count
    right_block = kernel.shape[1]
    factor_rows = lax.all_gather(factors, "rank", axis=1, tiled=True)
    factor_full = lax.all_gather(factor_rows, "vpair", axis=0, tiled=True)
    factor_cols = lax.dynamic_slice_in_dim(
        factor_full, lax.axis_index("rank") * right_block, right_block, 1
    )
    half_done = jnp.einsum(
        "ons,sh->onh",
        lax.all_gather(amplitudes, "rank", axis=2, tiled=True),
        factor_cols,
        preferred_element_type=jnp.float32,
    ).astype(jnp.bfloat16)
    kernel_sub = lax.all_to_all(kernel, "vpair", split_axis=1, concat_axis=0, tiled=True).astype(
        jnp.float32
    )
    coupled = jnp.einsum(
        "cp,icq->ipq",
        factor_full,
        lax.all_to_all(half_done, "vpair", split_axis=2, concat_axis=1, tiled=True),
        preferred_element_type=jnp.float32,
    )
    weighted = (kernel_sub[None] * coupled).astype(jnp.bfloat16)
    ladder_half = jnp.einsum(
        "ap,ipq->iaq", factor_full, weighted, preferred_element_type=jnp.float32
    ).astype(jnp.bfloat16)
    back_half = lax.all_to_all(ladder_half, "vpair", split_axis=1, concat_axis=2, tiled=True)
    partial_value = jnp.einsum(
        "iaq,bq->iab", back_half, factor_cols, preferred_element_type=jnp.float32
    )
    row_energy = lax.dynamic_slice_in_dim(
        virt_energy, lax.axis_index("vpair") * row_block, row_block, 0
    )
    ladder_share = lax.psum_scatter(partial_value, "rank", scatter_dimension=2, tiled=True)
    col_start = lax.axis_index("rank") * col_block
    own_terms = lax.dynamic_slice_in_dim(other_terms, col_start, col_block, 2)
    part_residual = own_terms + ladder_share
    col_energy = lax.dynamic_slice_in_dim(virt_energy, col_start, col_block, 0)
    denominator = row_energy[None, :, None] + col_energy[None, None, :] - pair_energy[:, None, None]
    update = part_residual / denominator
    squares = lax.psum(jnp.sum(update * update), ("vpair", "rank"))
    residual = lax.all_gather(part_residual, "rank", axis=2, tiled=True)
    update_rms = jnp.sqrt(squares / (pair_count * virt_count * virt_count) + epsilon)
    return (residual, update_rms)


MESH_IDS = pl.DeviceIdType.MESH


def middle_kernel(
    zs, own_ref, cols_ref, half_ref, kern_ref, out_ref, fall, hrecv, hturn, kturn, acc,
    loc_sem, hs, hr, fr, mr, zsend, xsend, msend, bs, br,
):
    v = lax.axis_index("vpair")
    r = lax.axis_index("rank")
    y, x = v // 2, v % 2
    z, core = r // 2, r % 2
    vx, vy, vd = y * 2 + 1 - x, (1 - y) * 2 + x, (1 - y) * 2 + 1 - x
    near = (vx, vy, vd)
    mate = z * 2 + 1 - core
    pairs, count, block, cols = hrecv.shape
    depth = own_ref.shape[1]
    rows = count * block
    group = 2
    groups = pairs // group
    tall = group * cols

    def rank_at(k, side):
        return ((z + k) % zs) * 2 + side

    barrier = pltpu.get_barrier_semaphore()
    peers = [(v, rank_at(k, core)) for k in range(1, zs)] + [(at, r) for at in near] + [(v, mate)]
    for peer in peers:
        pl.semaphore_signal(barrier, inc=1, device_id=peer, device_id_type=MESH_IDS)
    pl.semaphore_wait(barrier, len(peers))

    def remote(src, dst, send_sem, recv_sem, to):
        return pltpu.make_async_remote_copy(
            src_ref=src, dst_ref=dst, send_sem=send_sem, recv_sem=recv_sem,
            device_id=to, device_id_type=MESH_IDS,
        )

    def half_copy(i, j):
        at = pl.multiple_of(near[j] * cols, cols)
        return remote(
            half_ref.at[i, :, pl.ds(at, cols)], hrecv.at[i, v], hs.at[i, j], hr.at[i, v], (near[j], r)
        )

    def own_half(i):
        at = pl.multiple_of(v * cols, cols)
        return pltpu.make_async_copy(half_ref.at[i, :, pl.ds(at, cols)], hrecv.at[i, v], hr.at[i, v])

    def rows_copy(k):
        return remote(own_ref, fall.at[r, v], zsend.at[k], fr.at[r, v], (v, rank_at(k, core)))

    def side_copy(rr, at, k, j, to):
        return remote(fall.at[rr, at], fall.at[rr, at], xsend.at[k, j], fr.at[rr, at], (to, r))

    def mate_copy(k):
        rr = rank_at(k, core)
        return remote(fall.at[rr], fall.at[rr], msend.at[k], mr.at[rr], (v, mate))

    def shard_wait(rr, at):
        pltpu.make_async_copy(fall.at[rr, at], fall.at[rr, at], fr.at[rr, at]).wait()

    def block_wait(rr):
        pltpu.make_async_copy(fall.at[rr], fall.at[rr], mr.at[rr]).wait()

    def spread(k):
        rr = rank_at(k, core)
        shard_wait(rr, v)
        side_copy(rr, v, k, 0, vx).start()
        side_copy(rr, v, k, 1, vy).start()

    def relay_copy(k):
        rr = rank_at(k, core)
        odd = (rr // 2) % 2
        via = (y + odd * (1 - 2 * y)) * 2 + x + (1 - odd) * (1 - 2 * x)
        to = (y + (1 - odd) * (1 - 2 * y)) * 2 + x + odd * (1 - 2 * x)
        return side_copy(rr, via, k, 2, to)

    def relay(k):
        rr = rank_at(k, core)
        shard_wait(rr, vx)
        shard_wait(rr, vy)
        relay_copy(k).start()

    def finish(k):
        shard_wait(rank_at(k, core), vd)
        mate_copy(k).start()

    own_block = pltpu.make_async_copy(cols_ref, fall.at[r], loc_sem.at[0])
    mate_block = remote(cols_ref, fall.at[r], msend.at[0], mr.at[r], (v, mate))
    own_block.start()
    mate_block.start()
    for k in range(1, zs):
        rows_copy(k).start()

    @pl.loop(0, pairs)
    def _(i):
        for j in (0, 1, 2):
            half_copy(i, j).start()
        own_half(i).start()

    def turn_kernel(rr, slot):
        start = pl.multiple_of(rr * depth, depth)
        kturn[slot] = kern_ref[pl.ds(start, depth), :].T

    def compute(rr, slot, g):
        at = pl.multiple_of(g * tall, tall)
        shard = fall[rr].reshape(rows, depth)
        coupled = jnp.dot(hturn[pl.ds(at, tall), :], shard, preferred_element_type=jnp.float32)
        weight = kturn[slot].astype(jnp.float32)
        weighted = (coupled.reshape(group, cols, depth) * weight[None]).astype(jnp.bfloat16)
        return lax.dot_general(
            weighted.reshape(tall, depth), shard, (((1,), (1,)), ((), ())),
            preferred_element_type=jnp.float32,
        )

    turn_kernel(r, 0)
    turn_kernel(mate, 1)
    own_block.wait()
    block_wait(mate)

    @pl.loop(0, groups)
    def _(g):
        at = pl.multiple_of(g * tall, tall)
        for e in range(group):
            i = g * group + e
            for j in range(count):
                pltpu.make_async_copy(hrecv.at[i, j], hrecv.at[i, j], hr.at[i, j]).wait()
            hturn[pl.ds(at + e * cols, cols), :] = hrecv[i].reshape(rows, cols).T
        acc[pl.ds(at, tall), :] = compute(r, 0, g)
        acc[pl.ds(at, tall), :] += compute(mate, 1, g)

        @pl.when(g == 1)
        def _():
            spread(1)

    relay(1)
    spread(2)
    finish(1)

    @pl.loop(0, 2)
    def _(odd):
        rr = rank_at(1, core + odd - 2 * odd * core)

        @pl.when(odd == 1)
        def _():
            block_wait(rr)

        turn_kernel(rr, 0)

        @pl.loop(0, groups)
        def _(g):
            @pl.when(jnp.logical_and(odd == 0, g == 3))
            def _():
                relay(2)
                spread(3)

            @pl.when(jnp.logical_and(odd == 1, g == 2))
            def _():
                finish(2)

            at = pl.multiple_of(g * tall, tall)
            acc[pl.ds(at, tall), :] += compute(rr, 0, g)

    @pl.loop(0, 4)
    def _(n):
        side = n % 2
        turn_kernel(rank_at(n // 2 + 2, core + side - 2 * side * core), n)

    def back_copy(i, j):
        return remote(hrecv.at[i, near[j]], out_ref.at[i, v], bs.at[i, j], br.at[i, v], (near[j], r))

    def own_back(i):
        return pltpu.make_async_copy(hrecv.at[i, v], out_ref.at[i, v], br.at[i, v])

    @pl.loop(0, 2 * groups)
    def _(m):
        early = m < 4
        g = jnp.where(early, m % 2, m // 2)
        k = jnp.where(early, m // 2, m % 2) + 2

        @pl.when(m == 0)
        def _():
            block_wait(rank_at(2, 1 - core))

        @pl.when(m == 1)
        def _():
            relay(3)

        @pl.when(m == 2)
        def _():
            finish(3)

        at = pl.multiple_of(g * tall, tall)

        @pl.loop(0, 2)
        def _(side):
            @pl.when(jnp.logical_and(m == 2, side == 1))
            def _():
                block_wait(rank_at(3, 1 - core))

            rr = rank_at(k, core + side - 2 * side * core)
            acc[pl.ds(at, tall), :] += compute(rr, (k - 2) * 2 + side, g)

        @pl.when(k == 3)
        def _():
            for e in range(group):
                i = g * group + e
                piece = acc[pl.ds(at + e * cols, cols), :].astype(jnp.bfloat16)
                hrecv[i] = piece.T.reshape(count, block, cols)
                for j in (0, 1, 2):
                    back_copy(i, j).start()
                own_back(i).start()

    mate_block.wait_send()
    for k in range(1, zs):
        rows_copy(k).wait_send()
        side_copy(r, v, k, 0, vx).wait_send()
        side_copy(r, v, k, 1, vy).wait_send()
        relay_copy(k).wait_send()
        mate_copy(k).wait_send()

    @pl.loop(0, pairs)
    def _(i):
        for j in (0, 1, 2):
            half_copy(i, j).wait_send()
            back_copy(i, j).wait_send()
        for j in range(count):
            pltpu.make_async_copy(out_ref.at[i, j], out_ref.at[i, j], br.at[i, j]).wait()


def front_kernel(zs, own_ref, amp_ref, cols_ref, amps_ref, mine_sem, cols_recv, amps_recv, cs, us, ds, ms, stage, hold):
    v = lax.axis_index("vpair")
    r = lax.axis_index("rank")
    y, x = v // 2, v % 2
    z, core = r // 2, r % 2
    near = (y * 2 + 1 - x, (1 - y) * 2 + x, (1 - y) * 2 + 1 - x)
    mate = z * 2 + 1 - core
    mesh_ids = pl.DeviceIdType.MESH
    has_up, has_down = z + 1 < zs, z >= 1
    up_to, down_to = ((z + 1) % zs) * 2 + core, ((z + zs - 1) % zs) * 2 + core

    barrier = pltpu.get_barrier_semaphore()
    peers = [(at, r) for at in near] + [(v, mate), (v, up_to), (v, down_to)]
    for peer in peers:
        pl.semaphore_signal(barrier, inc=1, device_id=peer, device_id_type=mesh_ids)
    pl.semaphore_wait(barrier, len(peers))

    def cols_copy(j, at, to):
        return pltpu.make_async_remote_copy(
            src_ref=own_ref, dst_ref=cols_ref.at[at], send_sem=cs.at[j], recv_sem=cols_recv.at[at],
            device_id=(to, r), device_id_type=mesh_ids,
        )

    def amps_copy(src, at, sem, to):
        return pltpu.make_async_remote_copy(
            src_ref=src, dst_ref=amps_ref.at[at], send_sem=sem, recv_sem=amps_recv.at[at],
            device_id=(v, to), device_id_type=mesh_ids,
        )

    def amps_wait(at):
        pltpu.make_async_copy(amps_ref.at[at], amps_ref.at[at], amps_recv.at[at]).wait()

    @pl.when(has_up)
    def _():
        amps_copy(amp_ref, r, us.at[0], up_to).start()

    @pl.when(has_down)
    def _():
        amps_copy(amp_ref, r, ds.at[0], down_to).start()

    for j in range(3):
        cols_copy(j, v, near[j]).start()
    amps_copy(amp_ref, r, ms.at[0, 0], mate).start()
    a = pltpu.make_async_copy(own_ref, stage, mine_sem.at[0])
    b = pltpu.make_async_copy(amp_ref, hold, mine_sem.at[1])
    a.start()
    b.start()
    a.wait()
    b.wait()
    c = pltpu.make_async_copy(stage, cols_ref.at[v], mine_sem.at[2])
    d = pltpu.make_async_copy(hold, amps_ref.at[r], mine_sem.at[3])
    c.start()
    d.start()
    c.wait()
    d.wait()

    for s in range(1, zs):
        low, high = ((z + zs - s) % zs) * 2 + core, ((z + s) % zs) * 2 + core

        @pl.when(z >= s)
        def _():
            amps_wait(low)
            amps_copy(amps_ref.at[low], low, ms.at[s, 0], mate).start()

            @pl.when(has_up)
            def _():
                amps_copy(amps_ref.at[low], low, us.at[s], up_to).start()

        @pl.when(z + s < zs)
        def _():
            amps_wait(high)
            amps_copy(amps_ref.at[high], high, ms.at[s, 1], mate).start()

            @pl.when(has_down)
            def _():
                amps_copy(amps_ref.at[high], high, ds.at[s], down_to).start()

    for at in near:
        pltpu.make_async_copy(cols_ref.at[at], cols_ref.at[at], cols_recv.at[at]).wait()
    for k in range(zs):
        amps_wait(k * 2 + 1 - core)
    for j in range(3):
        cols_copy(j, v, near[j]).wait_send()
    amps_copy(amp_ref, r, ms.at[0, 0], mate).wait_send()
    for s in range(zs):

        @pl.when(jnp.logical_and(z >= s, has_up))
        def _():
            amps_copy(amp_ref, r, us.at[s], up_to).wait_send()

        @pl.when(jnp.logical_and(z + s < zs, has_down))
        def _():
            amps_copy(amp_ref, r, ds.at[s], down_to).wait_send()

        if s:

            @pl.when(z >= s)
            def _():
                amps_copy(amp_ref, r, ms.at[s, 0], mate).wait_send()

            @pl.when(z + s < zs)
            def _():
                amps_copy(amp_ref, r, ms.at[s, 1], mate).wait_send()


def front_gather(factors_pad, amps_pad, vpair_count, rank_count):
    zs = rank_count // 2
    hbm = pl.BlockSpec(memory_space=pl.ANY)
    return pl.pallas_call(
        functools.partial(front_kernel, zs),
        out_shape=(
            jax.ShapeDtypeStruct((vpair_count, *factors_pad.shape), jnp.bfloat16),
            jax.ShapeDtypeStruct((rank_count, *amps_pad.shape), jnp.bfloat16),
        ),
        in_specs=[hbm, hbm],
        out_specs=(hbm, hbm),
        scratch_shapes=[
            pltpu.SemaphoreType.DMA((4,)),
            pltpu.SemaphoreType.DMA((vpair_count,)),
            pltpu.SemaphoreType.DMA((rank_count,)),
            pltpu.SemaphoreType.DMA((3,)),
            pltpu.SemaphoreType.DMA((zs,)),
            pltpu.SemaphoreType.DMA((zs,)),
            pltpu.SemaphoreType.DMA((zs, 2)),
            pltpu.VMEM(factors_pad.shape, jnp.bfloat16),
            pltpu.VMEM(amps_pad.shape, jnp.bfloat16),
        ],
        compiler_params=pltpu.CompilerParams(
            collective_id=1, has_side_effects=True, vmem_limit_bytes=60 * 1024 * 1024
        ),
        cost_estimate=pl.CostEstimate(flops=10**10, bytes_accessed=10**7, transcendentals=0),
    )(factors_pad, amps_pad)


def ladder_middle(factors_pad, cols_pad, half_done, kernel_sub, rank_count):
    count, block, depth = cols_pad.shape
    pairs = half_done.shape[0]
    cols = kernel_sub.shape[1]
    rows = count * block
    points = kernel_sub.shape[0]
    zs = rank_count // 2
    hbm = pl.BlockSpec(memory_space=pl.ANY)
    vmem = pl.BlockSpec(memory_space=pltpu.VMEM)
    dma = pltpu.SemaphoreType.DMA
    return pl.pallas_call(
        functools.partial(middle_kernel, zs),
        out_shape=jax.ShapeDtypeStruct((pairs, count, block, cols), jnp.bfloat16),
        in_specs=[hbm, hbm, hbm, vmem],
        out_specs=hbm,
        scratch_shapes=[
            pltpu.VMEM((rank_count, count, block, depth), jnp.bfloat16),
            pltpu.VMEM((pairs, count, block, cols), jnp.bfloat16),
            pltpu.VMEM((pairs * cols, rows), jnp.bfloat16),
            pltpu.VMEM((4, cols, depth), jnp.bfloat16),
            pltpu.VMEM((pairs * cols, rows), jnp.float32),
            dma((1,)),
            dma((pairs, 3)),
            dma((pairs, count)),
            dma((rank_count, count)),
            dma((rank_count,)),
            dma((zs,)),
            dma((zs, 3)),
            dma((zs,)),
            dma((pairs, 3)),
            dma((pairs, count)),
        ],
        compiler_params=pltpu.CompilerParams(
            collective_id=0, has_side_effects=True, vmem_limit_bytes=62 * 1024 * 1024
        ),
        cost_estimate=pl.CostEstimate(
            flops=4 * pairs * points * rows * cols, bytes_accessed=4 * points * rows, transcendentals=0
        ),
    )(factors_pad, cols_pad, half_done, kernel_sub)


CUTS = 4


def tail_kernel(
    back_ref, cols_ref, other_ref, rowen_ref, virt_ref, res_ref, sq_ref,
    turned, part, msend, mrecv, zsend, outer, inner, fin, oth, sq, sqall,
    ms, mr, zs_sem, outr, inr, fs, fr, osem, rsem, qs, qr,
):
    v = lax.axis_index("vpair")
    r = lax.axis_index("rank")
    y, x = v // 2, v % 2
    z, core = r // 2, r % 2
    near = (y * 2 + 1 - x, (1 - y) * 2 + x, (1 - y) * 2 + 1 - x)
    mate = z * 2 + 1 - core
    pairs, count, block, cols = back_ref.shape
    rows = part.shape[1]
    turns = pairs // 2
    step_rows = -(-rows // (16 * CUTS)) * 16
    cuts = [(h * step_rows, min(step_rows, rows - h * step_rows)) for h in range(CUTS)]
    at_end = jnp.logical_or(z == 0, z == 3)
    in_middle = jnp.logical_not(at_end)
    toward_at = (v, jnp.where(z < 2, z + 1, z - 1) * 2 + core)
    away_at = (v, jnp.where(z == 1, 0, 3) * 2 + core)
    mate_at = (v, mate)

    barrier = pltpu.get_barrier_semaphore()
    for peer in [(at, r) for at in near] + [mate_at, toward_at]:
        pl.semaphore_signal(barrier, inc=1, device_id=peer, device_id_type=MESH_IDS)

    @pl.when(in_middle)
    def _():
        pl.semaphore_signal(barrier, inc=1, device_id=away_at, device_id_type=MESH_IDS)
        pl.semaphore_wait(barrier, 6)

    @pl.when(at_end)
    def _():
        pl.semaphore_wait(barrier, 5)

    def remote(src, dst, send_sem, recv_sem, to):
        return pltpu.make_async_remote_copy(
            src_ref=src, dst_ref=dst, send_sem=send_sem, recv_sem=recv_sem,
            device_id=to, device_id_type=MESH_IDS,
        )

    def arrive(ref, sem):
        pltpu.make_async_copy(ref, ref, sem).wait()

    def other_copy(p):
        return pltpu.make_async_copy(other_ref.at[:, p], oth.at[p], osem.at[p])

    def cut(ref, t, h):
        return ref.at[t, pl.ds(*cuts[h]), :]

    def read(ref, t, h):
        return ref[t, pl.ds(*cuts[h]), :].astype(jnp.float32)

    def res_copy(p, h):
        return pltpu.make_async_copy(cut(oth, p, h), res_ref.at[pl.ds(*cuts[h]), p], rsem.at[p, h])

    def mate_copy(t):
        return remote(msend.at[t], mrecv.at[t], ms.at[t], mr.at[t], mate_at)

    def outer_copy(t, h):
        return remote(cut(zsend, t, h), cut(outer, t, h), zs_sem.at[t, h], outr.at[t, h], toward_at)

    def inner_copy(t, h):
        return remote(cut(zsend, t, h), cut(inner, t, h), zs_sem.at[t, h], inr.at[t, h], toward_at)

    def fin_copy(p, h, j, to):
        return remote(cut(fin, p, h), cut(fin, p, h), fs.at[p // 2, h, j], fr.at[p, h], to)

    def ladder(p):
        left = jnp.concatenate([back_ref[p, j] for j in range(count)], axis=1)
        return jnp.dot(left, turned[...], preferred_element_type=jnp.float32)[:rows]

    def make(t):
        msend[t] = ladder(2 * t + 1 - core).astype(jnp.bfloat16)
        mate_copy(t).start()
        part[t] = ladder(2 * t + core)

    def give(t, h):
        if h == 0:
            arrive(mrecv.at[t], mr.at[t])

        @pl.when(at_end)
        def _():
            zsend[t, pl.ds(*cuts[h]), :] = (read(part, t, h) + read(mrecv, t, h)).astype(jnp.bfloat16)
            outer_copy(t, h).start()

    def meet(t, h):
        @pl.when(in_middle)
        def _():
            arrive(cut(outer, t, h), outr.at[t, h])
            both = read(part, t, h) + read(mrecv, t, h)
            zsend[t, pl.ds(*cuts[h]), :] = (both + read(outer, t, h)).astype(jnp.bfloat16)
            inner_copy(t, h).start()

    def close(t, h):
        p = 2 * t + core

        @pl.when(in_middle)
        def _():
            arrive(cut(inner, t, h), inr.at[t, h])
            fin[p, pl.ds(*cuts[h]), :] = (read(zsend, t, h) + read(inner, t, h)).astype(jnp.bfloat16)
            fin_copy(p, h, 0, away_at).start()
            fin_copy(p, h, 1, mate_at).start()

    def land(t, h):
        p = 2 * t + core

        @pl.when(at_end)
        def _():
            arrive(cut(fin, p, h), fr.at[p, h])
            fin_copy(p, h, 1, mate_at).start()

    def settle(t, h):
        q = 2 * t + 1 - core
        arrive(cut(fin, q, h), fr.at[q, h])
        for e in range(2):
            p = 2 * t + e
            if h == 0:
                other_copy(p).wait()
            value = read(oth, p, h) + read(fin, p, h)
            oth[p, pl.ds(*cuts[h]), :] = value
            update = value / (rowen_ref[p, pl.ds(*cuts[h]), :] + virt_ref[...])
            squares = jnp.sum(update * update, axis=0, keepdims=True)
            if h == 0:
                sq[pl.ds(p, 1), :] = squares
            else:
                sq[pl.ds(p, 1), :] += squares
            res_copy(p, h).start()

    @pl.loop(0, pairs)
    def _(p):
        other_copy(p).start()

    turned[...] = cols_ref[...].T
    stages = ((1, give), (3, meet), (5, close), (7, land), (8, settle))
    last = stages[-1][0]

    @pl.loop(0, turns + -(-last // CUTS))
    def _(u):
        @pl.when(u < turns)
        def _():
            make(u)

        for h in range(CUTS):
            for lag, stage in stages:
                t = u + (h - lag) // CUTS

                @pl.when(jnp.logical_and(t >= 0, t < turns))
                def _():
                    stage(t, (h - lag) % CUTS)

    sqall[v] = sq[...]
    for j in range(3):
        remote(sq, sqall.at[v], qs.at[j], qr.at[v], (near[j], r)).start()
    for at in near:
        arrive(sqall.at[at], qr.at[at])
    total = (sqall[0] + sqall[1]) + (sqall[2] + sqall[3])
    sq_ref[...] = jnp.sum(jnp.sum(total, axis=1, keepdims=True), axis=0, keepdims=True)

    for j in range(3):
        remote(sq, sqall.at[v], qs.at[j], qr.at[v], (near[j], r)).wait_send()

    @pl.loop(0, turns)
    def _(t):
        mate_copy(t).wait_send()
        for h in range(CUTS):
            outer_copy(t, h).wait_send()
            fin_copy(2 * t + core, h, 1, mate_at).wait_send()

            @pl.when(in_middle)
            def _():
                fin_copy(2 * t + core, h, 0, away_at).wait_send()

            for e in range(2):
                res_copy(2 * t + e, h).wait()


def ladder_tail(back, cols_flat, other_turned, row_energy, virt_energy):
    pairs, count, block, cols = back.shape
    rows = other_turned.shape[0]
    virt_count, depth = cols_flat.shape
    turns = pairs // 2
    hbm = pl.BlockSpec(memory_space=pl.ANY)
    vmem = pl.BlockSpec(memory_space=pltpu.VMEM)
    dma = pltpu.SemaphoreType.DMA
    bf16 = lambda *shape: pltpu.VMEM(shape, jnp.bfloat16)
    f32 = lambda *shape: pltpu.VMEM(shape, jnp.float32)
    return pl.pallas_call(
        tail_kernel,
        out_shape=(
            jax.ShapeDtypeStruct((rows, pairs, virt_count), jnp.float32),
            jax.ShapeDtypeStruct((1, 1), jnp.float32),
        ),
        in_specs=[vmem, vmem, hbm, vmem, vmem],
        out_specs=(hbm, vmem),
        scratch_shapes=[
            bf16(depth, virt_count),
            f32(turns, rows, virt_count),
            bf16(turns, rows, virt_count),
            bf16(turns, rows, virt_count),
            bf16(turns, rows, virt_count),
            bf16(turns, rows, virt_count),
            bf16(turns, rows, virt_count),
            bf16(pairs, rows, virt_count),
            f32(pairs, rows, virt_count),
            f32(pairs, virt_count),
            f32(count, pairs, virt_count),
            dma((turns,)),
            dma((turns,)),
            dma((turns, CUTS)),
            dma((turns, CUTS)),
            dma((turns, CUTS)),
            dma((turns, CUTS, 2)),
            dma((pairs, CUTS)),
            dma((pairs,)),
            dma((pairs, CUTS)),
            dma((3,)),
            dma((count,)),
        ],
        compiler_params=pltpu.CompilerParams(
            collective_id=2, has_side_effects=True, vmem_limit_bytes=62 * 1024 * 1024
        ),
        cost_estimate=pl.CostEstimate(
            flops=2 * pairs * rows * virt_count * depth, bytes_accessed=8 * pairs * rows * virt_count,
            transcendentals=0,
        ),
    )(back, cols_flat, other_turned, row_energy, virt_energy)


def fast_shards(amplitudes, factors, kernel, other_terms, virt_energy, pair_energy):
    vpair_count = lax.axis_size("vpair")
    rank_count = lax.axis_size("rank")
    pair_count, row_block, _ = amplitudes.shape
    virt_count = row_block * vpair_count
    right_block = kernel.shape[1]
    block = -(-row_block // 16) * 16
    col_block = amplitudes.shape[2]
    deep = -(-col_block // 16) * 16
    kernel_sub = lax.all_to_all(kernel, "vpair", split_axis=1, concat_axis=0, tiled=True)
    factors_pad = jnp.pad(factors, ((0, block - row_block), (0, 0)))
    amps_pad = jnp.pad(
        amplitudes.transpose(2, 0, 1), ((0, deep - col_block), (0, 0), (0, block - row_block))
    ).reshape(deep, pair_count * block)
    cols_pad, amps = front_gather(factors_pad, amps_pad, vpair_count, rank_count)
    factor_cols = cols_pad[:, :row_block].reshape(virt_count, right_block)
    cols_deep = jnp.pad(
        factor_cols.reshape(rank_count, col_block, right_block), ((0, 0), (0, deep - col_block), (0, 0))
    ).reshape(rank_count * deep, right_block)
    half_done = jnp.einsum(
        "sm,sh->mh",
        amps.reshape(rank_count * deep, pair_count * block),
        cols_deep,
        preferred_element_type=jnp.float32,
    ).astype(jnp.bfloat16)
    half_done = half_done.reshape(pair_count, block, right_block)
    back = ladder_middle(factors_pad, cols_pad, half_done, kernel_sub, rank_count)
    row_energy = lax.dynamic_slice_in_dim(
        virt_energy, lax.axis_index("vpair") * row_block, row_block, 0
    )
    shifted = row_energy[None, :, None] - pair_energy[:, None, None]
    residual, squares = ladder_tail(
        back, factor_cols, other_terms.transpose(1, 0, 2), shifted, virt_energy[None, :]
    )
    update_rms = jnp.sqrt(squares[0, 0] / (pair_count * virt_count * virt_count) + epsilon)
    return (residual.transpose(1, 0, 2), update_rms)


def pick(amplitudes, factors, kernel, other_terms, virt_energy, pair_energy):
    vpair_count = lax.axis_size("vpair")
    rank_count = lax.axis_size("rank")
    fits = (
        vpair_count == 4
        and rank_count == 8
        and amplitudes.shape[0] == 8
        and kernel.shape[1] % (128 * vpair_count) == 0
    )
    body = fast_shards if fits else shards
    return body(amplitudes, factors, kernel, other_terms, virt_energy, pair_energy)


def solution(mesh):
    placed = (
        P(None, "vpair", "rank"),
        P("vpair", "rank"),
        P("vpair", "rank"),
        P(None, "vpair", None),
        P(),
        P(),
    )
    return jax.shard_map(
        pick, mesh=mesh, in_specs=placed, out_specs=(P(None, "vpair", None), P()), check_vma=False
    )
```

```python
import functools

import jax
import jax.numpy as jnp
from jax import lax
from jax.experimental import pallas as pl
from jax.experimental.pallas import tpu as pltpu
from jax.sharding import PartitionSpec as P

epsilon = 1e-06


def shards(amplitudes, factors, kernel, other_terms, virt_energy, pair_energy):
    vpair_count = lax.axis_size("vpair")
    pair_count = amplitudes.shape[0]
    row_block = amplitudes.shape[1]
    col_block = amplitudes.shape[2]
    virt_count = row_block * vpair_count
    right_block = kernel.shape[1]
    factor_rows = lax.all_gather(factors, "rank", axis=1, tiled=True)
    factor_full = lax.all_gather(factor_rows, "vpair", axis=0, tiled=True)
    factor_cols = lax.dynamic_slice_in_dim(
        factor_full, lax.axis_index("rank") * right_block, right_block, 1
    )
    half_done = jnp.einsum(
        "ons,sh->onh",
        lax.all_gather(amplitudes, "rank", axis=2, tiled=True),
        factor_cols,
        preferred_element_type=jnp.float32,
    ).astype(jnp.bfloat16)
    kernel_sub = lax.all_to_all(kernel, "vpair", split_axis=1, concat_axis=0, tiled=True).astype(
        jnp.float32
    )
    coupled = jnp.einsum(
        "cp,icq->ipq",
        factor_full,
        lax.all_to_all(half_done, "vpair", split_axis=2, concat_axis=1, tiled=True),
        preferred_element_type=jnp.float32,
    )
    weighted = (kernel_sub[None] * coupled).astype(jnp.bfloat16)
    ladder_half = jnp.einsum(
        "ap,ipq->iaq", factor_full, weighted, preferred_element_type=jnp.float32
    ).astype(jnp.bfloat16)
    back_half = lax.all_to_all(ladder_half, "vpair", split_axis=1, concat_axis=2, tiled=True)
    partial_value = jnp.einsum(
        "iaq,bq->iab", back_half, factor_cols, preferred_element_type=jnp.float32
    )
    row_energy = lax.dynamic_slice_in_dim(
        virt_energy, lax.axis_index("vpair") * row_block, row_block, 0
    )
    ladder_share = lax.psum_scatter(partial_value, "rank", scatter_dimension=2, tiled=True)
    col_start = lax.axis_index("rank") * col_block
    own_terms = lax.dynamic_slice_in_dim(other_terms, col_start, col_block, 2)
    part_residual = own_terms + ladder_share
    col_energy = lax.dynamic_slice_in_dim(virt_energy, col_start, col_block, 0)
    denominator = row_energy[None, :, None] + col_energy[None, None, :] - pair_energy[:, None, None]
    update = part_residual / denominator
    squares = lax.psum(jnp.sum(update * update), ("vpair", "rank"))
    residual = lax.all_gather(part_residual, "rank", axis=2, tiled=True)
    update_rms = jnp.sqrt(squares / (pair_count * virt_count * virt_count) + epsilon)
    return (residual, update_rms)


MESH_IDS = pl.DeviceIdType.MESH


def middle_kernel(
    zs, cols_ref, line_ref, half_ref, kern_ref, out_ref, fall, hrecv, hturn, kturn, acc,
    loc_sem, hr, fr, mr, xsend, msend, bs, br,
):
    v = lax.axis_index("vpair")
    r = lax.axis_index("rank")
    y, x = v // 2, v % 2
    z, core = r // 2, r % 2
    vx, vy, vd = y * 2 + 1 - x, (1 - y) * 2 + x, (1 - y) * 2 + 1 - x
    near = (vx, vy, vd)
    mate = z * 2 + 1 - core
    pairs, count, block, cols = hrecv.shape
    depth = cols_ref.shape[2]
    rows = count * block
    group = 2
    groups = pairs // group
    tall = group * cols

    def rank_at(k, side):
        return ((z + k) % zs) * 2 + side

    barrier = pltpu.get_barrier_semaphore()
    peers = [(at, r) for at in near] + [(v, mate)]
    for peer in peers:
        pl.semaphore_signal(barrier, inc=1, device_id=peer, device_id_type=MESH_IDS)
    pl.semaphore_wait(barrier, len(peers))

    def remote(src, dst, send_sem, recv_sem, to):
        return pltpu.make_async_remote_copy(
            src_ref=src, dst_ref=dst, send_sem=send_sem, recv_sem=recv_sem,
            device_id=to, device_id_type=MESH_IDS,
        )

    def own_half(i):
        return pltpu.make_async_copy(half_ref.at[i], hrecv.at[i], hr.at[i])

    def line_copy(k, slot):
        at = vd if slot else v
        rr = rank_at(k, core)
        return pltpu.make_async_copy(line_ref.at[rr // 2, slot], fall.at[rr, at], fr.at[rr, at])

    def side_copy(k, j):
        rr = rank_at(k, core)
        return remote(line_ref.at[rr // 2, 0], fall.at[rr, v], xsend.at[k, j], fr.at[rr, v], (near[j], r))

    def mate_copy(k):
        rr = rank_at(k, core)
        return remote(fall.at[rr], fall.at[rr], msend.at[k], mr.at[rr], (v, mate))

    def shard_wait(rr, at):
        pltpu.make_async_copy(fall.at[rr, at], fall.at[rr, at], fr.at[rr, at]).wait()

    def block_wait(rr):
        pltpu.make_async_copy(fall.at[rr], fall.at[rr], mr.at[rr]).wait()

    def finish(k):
        rr = rank_at(k, core)
        for at in (v, vx, vy, vd):
            shard_wait(rr, at)
        mate_copy(k).start()

    own_block = pltpu.make_async_copy(cols_ref, fall.at[r], loc_sem.at[0])
    mate_block = remote(cols_ref, fall.at[r], msend.at[0], mr.at[r], (v, mate))
    own_block.start()
    mate_block.start()
    for k in range(1, zs):
        for j in (0, 1):
            side_copy(k, j).start()

    @pl.loop(0, pairs)
    def _(i):
        own_half(i).start()

    for k in range(1, zs):
        for slot in (0, 1):
            line_copy(k, slot).start()

    def turn_kernel(rr, slot):
        start = pl.multiple_of(rr * depth, depth)
        kturn[slot] = kern_ref[pl.ds(start, depth), :].T

    def compute(rr, slot, g):
        at = pl.multiple_of(g * tall, tall)
        shard = fall[rr].reshape(rows, depth)
        coupled = jnp.dot(hturn[pl.ds(at, tall), :], shard, preferred_element_type=jnp.float32)
        weight = kturn[slot].astype(jnp.float32)
        weighted = (coupled.reshape(group, cols, depth) * weight[None]).astype(jnp.bfloat16)
        return lax.dot_general(
            weighted.reshape(tall, depth), shard, (((1,), (1,)), ((), ())),
            preferred_element_type=jnp.float32,
        )

    turn_kernel(r, 0)
    turn_kernel(mate, 1)
    own_block.wait()
    block_wait(mate)

    @pl.loop(0, groups)
    def _(g):
        at = pl.multiple_of(g * tall, tall)
        for e in range(group):
            i = g * group + e
            own_half(i).wait()
            hturn[pl.ds(at + e * cols, cols), :] = hrecv[i].reshape(rows, cols).T
        acc[pl.ds(at, tall), :] = compute(r, 0, g)
        acc[pl.ds(at, tall), :] += compute(mate, 1, g)

        @pl.when(g == 2)
        def _():
            finish(1)

    @pl.loop(0, 2)
    def _(odd):
        rr = rank_at(1, core + odd - 2 * odd * core)

        @pl.when(odd == 1)
        def _():
            block_wait(rr)

        turn_kernel(rr, 0)

        @pl.loop(0, groups)
        def _(g):
            @pl.when(jnp.logical_and(odd == 0, g == 2))
            def _():
                finish(2)

            @pl.when(jnp.logical_and(odd == 1, g == 2))
            def _():
                finish(3)

            at = pl.multiple_of(g * tall, tall)
            acc[pl.ds(at, tall), :] += compute(rr, 0, g)

    @pl.loop(0, 4)
    def _(n):
        side = n % 2
        turn_kernel(rank_at(n // 2 + 2, core + side - 2 * side * core), n)

    def back_copy(i, j):
        return remote(hrecv.at[i, near[j]], out_ref.at[i, v], bs.at[i, j], br.at[i, v], (near[j], r))

    def own_back(i):
        return pltpu.make_async_copy(hrecv.at[i, v], out_ref.at[i, v], br.at[i, v])

    @pl.loop(0, 2 * groups)
    def _(m):
        g = m // 2
        k = m % 2 + 2

        at = pl.multiple_of(g * tall, tall)

        @pl.loop(0, 2)
        def _(side):
            rr = rank_at(k, core + side - 2 * side * core)

            @pl.when(jnp.logical_and(g == 0, side == 1))
            def _():
                block_wait(rr)

            acc[pl.ds(at, tall), :] += compute(rr, (k - 2) * 2 + side, g)

        @pl.when(k == 3)
        def _():
            for e in range(group):
                i = g * group + e
                piece = acc[pl.ds(at + e * cols, cols), :].astype(jnp.bfloat16)
                hrecv[i] = piece.T.reshape(count, block, cols)
                for j in (0, 1, 2):
                    back_copy(i, j).start()
                own_back(i).start()

    mate_block.wait_send()
    for k in range(1, zs):
        for j in (0, 1):
            side_copy(k, j).wait_send()
        mate_copy(k).wait_send()

    @pl.loop(0, pairs)
    def _(i):
        for j in (0, 1, 2):
            back_copy(i, j).wait_send()
        for j in range(count):
            pltpu.make_async_copy(out_ref.at[i, j], out_ref.at[i, j], br.at[i, j]).wait()


def front_kernel(
    zs, col_block, own_ref, amp_ref, kern_ref, cols_ref, half_ref, z_ref, line_ref,
    cbuf, amps, zbuf, deep, hstage,
    mine, cs, cr, us, ds, ms, ar, ks, kr, hs, hr, lu, ld, lr,
):
    v = lax.axis_index("vpair")
    r = lax.axis_index("rank")
    y, x = v // 2, v % 2
    z, core = r // 2, r % 2
    near = (y * 2 + 1 - x, (1 - y) * 2 + x, (1 - y) * 2 + 1 - x)
    vd = near[2]
    mate = z * 2 + 1 - core
    has_up, has_down = z + 1 < zs, z >= 1
    up_to, down_to = ((z + 1) % zs) * 2 + core, ((z + zs - 1) % zs) * 2 + core
    pairs, count, block, cols = half_ref.shape
    points = kern_ref.shape[0]
    rank_count, deep_block = amps.shape[:2]
    groups = hstage.shape[0]
    wide = hstage.shape[1]
    group = pairs // groups

    barrier = pltpu.get_barrier_semaphore()
    peers = [(at, r) for at in near] + [(v, mate), (v, up_to), (v, down_to)]
    for peer in peers:
        pl.semaphore_signal(barrier, inc=1, device_id=peer, device_id_type=MESH_IDS)
    pl.semaphore_wait(barrier, len(peers))

    def remote(src, dst, send_sem, recv_sem, to):
        return pltpu.make_async_remote_copy(
            src_ref=src, dst_ref=dst, send_sem=send_sem, recv_sem=recv_sem,
            device_id=to, device_id_type=MESH_IDS,
        )

    def arrive(ref, sem):
        pltpu.make_async_copy(ref, ref, sem).wait()

    def amps_copy(src, at, sem, to):
        return remote(src, amps.at[at], sem, ar.at[at], (v, to))

    def cols_copy(j):
        return remote(own_ref, cbuf.at[v], cs.at[j], cr.at[v], (near[j], r))

    def part_of(at):
        return kern_ref.at[:, pl.ds(pl.multiple_of(at * cols, cols), cols)]

    def rows_of(at):
        return z_ref.at[pl.ds(pl.multiple_of(at * points, points), points), :]

    def kern_copy(j):
        return remote(part_of(near[j]), rows_of(v), ks.at[j], kr.at[v], (near[j], r))

    def line_copy(src, at, slot, sem, to):
        return remote(src, line_ref.at[at, slot], sem.at[at, slot], lr.at[at, slot], (v, to))

    def half_piece(i, at):
        rows_at = pl.multiple_of((i % group) * (wide // group), 16)
        return hstage.at[i // group, pl.ds(rows_at, block), pl.ds(pl.multiple_of(at * cols, cols), cols)]

    def half_copy(i, j):
        return remote(half_piece(i, near[j]), half_ref.at[i, v], hs.at[i, j], hr.at[i, v], (near[j], r))

    def own_half(i):
        return pltpu.make_async_copy(half_piece(i, v), half_ref.at[i, v], hr.at[i, v])

    @pl.when(has_up)
    def _():
        amps_copy(amp_ref, r, us.at[0], up_to).start()

    @pl.when(has_down)
    def _():
        amps_copy(amp_ref, r, ds.at[0], down_to).start()

    for j in (0, 1, 2):
        cols_copy(j).start()
    amps_copy(amp_ref, r, ms.at[0, 0], mate).start()
    for j in (0, 1, 2):
        kern_copy(j).start()
    own_cols = pltpu.make_async_copy(own_ref, cbuf.at[v], mine.at[0])
    own_amps = pltpu.make_async_copy(amp_ref, amps.at[r], mine.at[1])
    own_in = pltpu.make_async_copy(part_of(v), zbuf, mine.at[2])
    own_out = pltpu.make_async_copy(zbuf, rows_of(v), mine.at[2])
    own_cols.start()
    own_amps.start()
    own_in.start()
    deep[...] = jnp.zeros_like(deep)
    own_cols.wait()
    own_amps.wait()
    own_in.wait()
    own_out.start()

    def amps_step(s):
        low, high = ((z + zs - s) % zs) * 2 + core, ((z + s) % zs) * 2 + core

        @pl.when(z >= s)
        def _():
            arrive(amps.at[low], ar.at[low])
            amps_copy(amps.at[low], low, ms.at[s, 0], mate).start()

            @pl.when(has_up)
            def _():
                amps_copy(amps.at[low], low, us.at[s], up_to).start()

        @pl.when(z + s < zs)
        def _():
            arrive(amps.at[high], ar.at[high])
            amps_copy(amps.at[high], high, ms.at[s, 1], mate).start()

            @pl.when(has_down)
            def _():
                amps_copy(amps.at[high], high, ds.at[s], down_to).start()

    def line_step(s):
        low, high = (z + zs - s) % zs, (z + s) % zs

        @pl.when(z >= s)
        def _():
            for slot in (0, 1):
                arrive(line_ref.at[low, slot], lr.at[low, slot])

                @pl.when(has_up)
                def _():
                    line_copy(line_ref.at[low, slot], low, slot, lu, up_to).start()

        @pl.when(z + s < zs)
        def _():
            for slot in (0, 1):
                arrive(line_ref.at[high, slot], lr.at[high, slot])

                @pl.when(has_down)
                def _():
                    line_copy(line_ref.at[high, slot], high, slot, ld, down_to).start()

    for s in range(1, zs - 1):
        amps_step(s)
    for at in near:
        arrive(cbuf.at[at], cr.at[at])
    cols_out = pltpu.make_async_copy(cbuf, cols_ref, mine.at[0])
    cols_out.start()

    @pl.when(has_up)
    def _():
        for slot, at in ((0, v), (1, vd)):
            line_copy(cbuf.at[at], z, slot, lu, up_to).start()

    @pl.when(has_down)
    def _():
        for slot, at in ((0, v), (1, vd)):
            line_copy(cbuf.at[at], z, slot, ld, down_to).start()

    per = rank_count // count
    for j in range(count):
        whole = cbuf[j]
        for e in range(per):
            at = (j * per + e) * deep_block
            deep[at : at + col_block, :] = whole[e * col_block : (e + 1) * col_block]
    amps_step(zs - 1)
    for k in range(zs):
        at = k * 2 + 1 - core
        arrive(amps.at[at], ar.at[at])

    @pl.loop(0, groups)
    def _(g):
        left = amps[:, :, pl.ds(pl.multiple_of(g * wide, wide), wide)].reshape(rank_count * deep_block, wide)
        done = lax.dot_general(
            left, deep[...], (((0,), (0,)), ((), ())), preferred_element_type=jnp.float32
        )
        hstage[g] = done.astype(jnp.bfloat16)
        for e in range(group):
            i = g * group + e
            for j in (0, 1, 2):
                half_copy(i, j).start()
            own_half(i).start()

    for s in range(1, zs):
        line_step(s)
    for at in near:
        arrive(rows_of(at), kr.at[at])

    @pl.loop(0, pairs)
    def _(i):
        for j in range(count):
            arrive(half_ref.at[i, j], hr.at[i, j])
        for j in (0, 1, 2):
            half_copy(i, j).wait_send()

    own_out.wait()
    cols_out.wait()
    for j in (0, 1, 2):
        cols_copy(j).wait_send()
        kern_copy(j).wait_send()
    amps_copy(amp_ref, r, ms.at[0, 0], mate).wait_send()

    def line_sent(at, sem, to):
        for slot in (0, 1):
            line_copy(cbuf.at[0], at, slot, sem, to).wait_send()

    for s in range(zs):
        @pl.when(jnp.logical_and(z >= s, has_up))
        def _():
            amps_copy(amp_ref, r, us.at[s], up_to).wait_send()
            line_sent((z + zs - s) % zs, lu, up_to)

        @pl.when(jnp.logical_and(z + s < zs, has_down))
        def _():
            amps_copy(amp_ref, r, ds.at[s], down_to).wait_send()
            line_sent((z + s) % zs, ld, down_to)

        if s:

            @pl.when(z >= s)
            def _():
                amps_copy(amp_ref, r, ms.at[s, 0], mate).wait_send()

            @pl.when(z + s < zs)
            def _():
                amps_copy(amp_ref, r, ms.at[s, 1], mate).wait_send()


def front_gather(factors_pad, amps_pad, kernel, pairs, col_block, vpair_count, rank_count):
    zs = rank_count // 2
    block, right_block = factors_pad.shape
    points = kernel.shape[0]
    cols = right_block // vpair_count
    deep_block, width = amps_pad.shape
    groups = pairs // 2
    hbm = pl.BlockSpec(memory_space=pl.ANY)
    dma = pltpu.SemaphoreType.DMA
    bf16 = lambda *shape: pltpu.VMEM(shape, jnp.bfloat16)
    like = lambda *shape: jax.ShapeDtypeStruct(shape, jnp.bfloat16)
    return pl.pallas_call(
        functools.partial(front_kernel, zs, col_block),
        out_shape=(
            like(vpair_count, block, right_block),
            like(pairs, vpair_count, block, cols),
            like(points * vpair_count, cols),
            like(zs, 2, block, right_block),
        ),
        in_specs=[hbm, hbm, hbm],
        out_specs=(hbm, hbm, hbm, hbm),
        scratch_shapes=[
            bf16(vpair_count, block, right_block),
            bf16(rank_count, deep_block, width),
            bf16(points, cols),
            bf16(rank_count * deep_block, right_block),
            bf16(groups, width // groups, right_block),
            dma((3,)),
            dma((3,)),
            dma((vpair_count,)),
            dma((zs,)),
            dma((zs,)),
            dma((zs, 2)),
            dma((rank_count,)),
            dma((3,)),
            dma((vpair_count,)),
            dma((pairs, 3)),
            dma((pairs, vpair_count)),
            dma((zs, 2)),
            dma((zs, 2)),
            dma((zs, 2)),
        ],
        compiler_params=pltpu.CompilerParams(
            collective_id=1, has_side_effects=True, vmem_limit_bytes=60 * 1024 * 1024
        ),
        cost_estimate=pl.CostEstimate(flops=10**10, bytes_accessed=10**7, transcendentals=0),
    )(factors_pad, amps_pad, kernel)


def ladder_middle(cols_pad, line, half, kernel_sub, rank_count):
    count, block, depth = cols_pad.shape
    pairs = half.shape[0]
    cols = kernel_sub.shape[1]
    rows = count * block
    points = kernel_sub.shape[0]
    zs = rank_count // 2
    hbm = pl.BlockSpec(memory_space=pl.ANY)
    vmem = pl.BlockSpec(memory_space=pltpu.VMEM)
    dma = pltpu.SemaphoreType.DMA
    return pl.pallas_call(
        functools.partial(middle_kernel, zs),
        out_shape=jax.ShapeDtypeStruct((pairs, count, block, cols), jnp.bfloat16),
        in_specs=[hbm, hbm, hbm, vmem],
        out_specs=hbm,
        scratch_shapes=[
            pltpu.VMEM((rank_count, count, block, depth), jnp.bfloat16),
            pltpu.VMEM((pairs, count, block, cols), jnp.bfloat16),
            pltpu.VMEM((pairs * cols, rows), jnp.bfloat16),
            pltpu.VMEM((4, cols, depth), jnp.bfloat16),
            pltpu.VMEM((pairs * cols, rows), jnp.float32),
            dma((1,)),
            dma((pairs,)),
            dma((rank_count, count)),
            dma((rank_count,)),
            dma((zs, 2)),
            dma((zs,)),
            dma((pairs, 3)),
            dma((pairs, count)),
        ],
        compiler_params=pltpu.CompilerParams(
            collective_id=0, has_side_effects=True, vmem_limit_bytes=62 * 1024 * 1024
        ),
        cost_estimate=pl.CostEstimate(
            flops=4 * pairs * points * rows * cols, bytes_accessed=4 * points * rows, transcendentals=0
        ),
    )(cols_pad, line, half, kernel_sub)


CUTS = 4


def tail_kernel(
    back_ref, cols_ref, other_ref, rowen_ref, virt_ref, res_ref, sq_ref,
    turned, part, msend, mrecv, zsend, outer, inner, fin, oth, sq, sqall,
    ms, mr, zs_sem, outr, inr, fs, fr, osem, rsem, qs, qr,
):
    v = lax.axis_index("vpair")
    r = lax.axis_index("rank")
    y, x = v // 2, v % 2
    z, core = r // 2, r % 2
    near = (y * 2 + 1 - x, (1 - y) * 2 + x, (1 - y) * 2 + 1 - x)
    mate = z * 2 + 1 - core
    pairs, count, block, cols = back_ref.shape
    rows = part.shape[1]
    turns = pairs // 2
    step_rows = -(-rows // (16 * CUTS)) * 16
    cuts = [(h * step_rows, min(step_rows, rows - h * step_rows)) for h in range(CUTS)]
    at_end = jnp.logical_or(z == 0, z == 3)
    in_middle = jnp.logical_not(at_end)
    toward_at = (v, jnp.where(z < 2, z + 1, z - 1) * 2 + core)
    away_at = (v, jnp.where(z == 1, 0, 3) * 2 + core)
    mate_at = (v, mate)

    barrier = pltpu.get_barrier_semaphore()
    for peer in [(at, r) for at in near] + [mate_at, toward_at]:
        pl.semaphore_signal(barrier, inc=1, device_id=peer, device_id_type=MESH_IDS)

    @pl.when(in_middle)
    def _():
        pl.semaphore_signal(barrier, inc=1, device_id=away_at, device_id_type=MESH_IDS)
        pl.semaphore_wait(barrier, 6)

    @pl.when(at_end)
    def _():
        pl.semaphore_wait(barrier, 5)

    def remote(src, dst, send_sem, recv_sem, to):
        return pltpu.make_async_remote_copy(
            src_ref=src, dst_ref=dst, send_sem=send_sem, recv_sem=recv_sem,
            device_id=to, device_id_type=MESH_IDS,
        )

    def arrive(ref, sem):
        pltpu.make_async_copy(ref, ref, sem).wait()

    def other_copy(p):
        return pltpu.make_async_copy(other_ref.at[:, p], oth.at[p], osem.at[p])

    def cut(ref, t, h):
        return ref.at[t, pl.ds(*cuts[h]), :]

    def read(ref, t, h):
        return ref[t, pl.ds(*cuts[h]), :].astype(jnp.float32)

    def res_copy(p, h):
        return pltpu.make_async_copy(cut(oth, p, h), res_ref.at[pl.ds(*cuts[h]), p], rsem.at[p, h])

    def mate_copy(t):
        return remote(msend.at[t], mrecv.at[t], ms.at[t], mr.at[t], mate_at)

    def outer_copy(t, h):
        return remote(cut(zsend, t, h), cut(outer, t, h), zs_sem.at[t, h], outr.at[t, h], toward_at)

    def inner_copy(t, h):
        return remote(cut(zsend, t, h), cut(inner, t, h), zs_sem.at[t, h], inr.at[t, h], toward_at)

    def fin_copy(p, h, j, to):
        return remote(cut(fin, p, h), cut(fin, p, h), fs.at[p // 2, h, j], fr.at[p, h], to)

    def ladder(p):
        left = jnp.concatenate([back_ref[p, j] for j in range(count)], axis=1)
        return jnp.dot(left, turned[...], preferred_element_type=jnp.float32)[:rows]

    def make(t):
        msend[t] = ladder(2 * t + 1 - core).astype(jnp.bfloat16)
        mate_copy(t).start()
        part[t] = ladder(2 * t + core)

    def give(t, h):
        if h == 0:
            arrive(mrecv.at[t], mr.at[t])

        @pl.when(at_end)
        def _():
            zsend[t, pl.ds(*cuts[h]), :] = (read(part, t, h) + read(mrecv, t, h)).astype(jnp.bfloat16)
            outer_copy(t, h).start()

    def meet(t, h):
        @pl.when(in_middle)
        def _():
            arrive(cut(outer, t, h), outr.at[t, h])
            both = read(part, t, h) + read(mrecv, t, h)
            zsend[t, pl.ds(*cuts[h]), :] = (both + read(outer, t, h)).astype(jnp.bfloat16)
            inner_copy(t, h).start()

    def close(t, h):
        p = 2 * t + core

        @pl.when(in_middle)
        def _():
            arrive(cut(inner, t, h), inr.at[t, h])
            fin[p, pl.ds(*cuts[h]), :] = (read(zsend, t, h) + read(inner, t, h)).astype(jnp.bfloat16)
            fin_copy(p, h, 0, away_at).start()
            fin_copy(p, h, 1, mate_at).start()

    def land(t, h):
        p = 2 * t + core

        @pl.when(at_end)
        def _():
            arrive(cut(fin, p, h), fr.at[p, h])
            fin_copy(p, h, 1, mate_at).start()

    def settle(t, h):
        q = 2 * t + 1 - core
        arrive(cut(fin, q, h), fr.at[q, h])
        for e in range(2):
            p = 2 * t + e
            if h == 0:
                other_copy(p).wait()
            value = read(oth, p, h) + read(fin, p, h)
            oth[p, pl.ds(*cuts[h]), :] = value
            update = value / (rowen_ref[p, pl.ds(*cuts[h]), :] + virt_ref[...])
            squares = jnp.sum(update * update, axis=0, keepdims=True)
            if h == 0:
                sq[pl.ds(p, 1), :] = squares
            else:
                sq[pl.ds(p, 1), :] += squares
            res_copy(p, h).start()

    @pl.loop(0, pairs)
    def _(p):
        other_copy(p).start()

    flat = jnp.concatenate([cols_ref[j, :rows, :] for j in range(count)], axis=0)
    turned[...] = flat.T
    stages = ((1, give), (3, meet), (5, close), (7, land), (8, settle))
    last = stages[-1][0]

    @pl.loop(0, turns + -(-last // CUTS))
    def _(u):
        @pl.when(u < turns)
        def _():
            make(u)

        for h in range(CUTS):
            for lag, stage in stages:
                t = u + (h - lag) // CUTS

                @pl.when(jnp.logical_and(t >= 0, t < turns))
                def _():
                    stage(t, (h - lag) % CUTS)

    sqall[v] = sq[...]
    for j in range(3):
        remote(sq, sqall.at[v], qs.at[j], qr.at[v], (near[j], r)).start()
    for at in near:
        arrive(sqall.at[at], qr.at[at])
    total = (sqall[0] + sqall[1]) + (sqall[2] + sqall[3])
    sq_ref[...] = jnp.sum(jnp.sum(total, axis=1, keepdims=True), axis=0, keepdims=True)

    for j in range(3):
        remote(sq, sqall.at[v], qs.at[j], qr.at[v], (near[j], r)).wait_send()

    @pl.loop(0, turns)
    def _(t):
        mate_copy(t).wait_send()
        for h in range(CUTS):
            outer_copy(t, h).wait_send()
            fin_copy(2 * t + core, h, 1, mate_at).wait_send()

            @pl.when(in_middle)
            def _():
                fin_copy(2 * t + core, h, 0, away_at).wait_send()

            for e in range(2):
                res_copy(2 * t + e, h).wait()


def ladder_tail(back, cols_pad, other_turned, row_energy, virt_energy):
    pairs, count, block, cols = back.shape
    rows = other_turned.shape[0]
    virt_count, depth = virt_energy.shape[1], cols_pad.shape[2]
    turns = pairs // 2
    hbm = pl.BlockSpec(memory_space=pl.ANY)
    vmem = pl.BlockSpec(memory_space=pltpu.VMEM)
    dma = pltpu.SemaphoreType.DMA
    bf16 = lambda *shape: pltpu.VMEM(shape, jnp.bfloat16)
    f32 = lambda *shape: pltpu.VMEM(shape, jnp.float32)
    return pl.pallas_call(
        tail_kernel,
        out_shape=(
            jax.ShapeDtypeStruct((rows, pairs, virt_count), jnp.float32),
            jax.ShapeDtypeStruct((1, 1), jnp.float32),
        ),
        in_specs=[vmem, vmem, hbm, vmem, vmem],
        out_specs=(hbm, vmem),
        scratch_shapes=[
            bf16(depth, virt_count),
            f32(turns, rows, virt_count),
            bf16(turns, rows, virt_count),
            bf16(turns, rows, virt_count),
            bf16(turns, rows, virt_count),
            bf16(turns, rows, virt_count),
            bf16(turns, rows, virt_count),
            bf16(pairs, rows, virt_count),
            f32(pairs, rows, virt_count),
            f32(pairs, virt_count),
            f32(count, pairs, virt_count),
            dma((turns,)),
            dma((turns,)),
            dma((turns, CUTS)),
            dma((turns, CUTS)),
            dma((turns, CUTS)),
            dma((turns, CUTS, 2)),
            dma((pairs, CUTS)),
            dma((pairs,)),
            dma((pairs, CUTS)),
            dma((3,)),
            dma((count,)),
        ],
        compiler_params=pltpu.CompilerParams(
            collective_id=2, has_side_effects=True, vmem_limit_bytes=62 * 1024 * 1024
        ),
        cost_estimate=pl.CostEstimate(
            flops=2 * pairs * rows * virt_count * depth, bytes_accessed=8 * pairs * rows * virt_count,
            transcendentals=0,
        ),
    )(back, cols_pad, other_turned, row_energy, virt_energy)


def fast_shards(amplitudes, factors, kernel, other_terms, virt_energy, pair_energy):
    vpair_count = lax.axis_size("vpair")
    rank_count = lax.axis_size("rank")
    pair_count, row_block, _ = amplitudes.shape
    virt_count = row_block * vpair_count
    block = -(-row_block // 16) * 16
    tall = -(-row_block // 64) * 64
    col_block = amplitudes.shape[2]
    deep = -(-col_block // 16) * 16
    factors_pad = jnp.pad(factors, ((0, block - row_block), (0, 0)))
    amps_pad = jnp.pad(
        amplitudes.transpose(2, 0, 1), ((0, deep - col_block), (0, 0), (0, tall - row_block))
    ).reshape(deep, pair_count * tall)
    cols_pad, half, kernel_sub, line = front_gather(
        factors_pad, amps_pad, kernel, pair_count, col_block, vpair_count, rank_count
    )
    back = ladder_middle(cols_pad, line, half, kernel_sub, rank_count)
    row_energy = lax.dynamic_slice_in_dim(
        virt_energy, lax.axis_index("vpair") * row_block, row_block, 0
    )
    shifted = row_energy[None, :, None] - pair_energy[:, None, None]
    residual, squares = ladder_tail(
        back, cols_pad, other_terms.transpose(1, 0, 2), shifted, virt_energy[None, :]
    )
    update_rms = jnp.sqrt(squares[0, 0] / (pair_count * virt_count * virt_count) + epsilon)
    return (residual.transpose(1, 0, 2), update_rms)


def pick(amplitudes, factors, kernel, other_terms, virt_energy, pair_energy):
    vpair_count = lax.axis_size("vpair")
    rank_count = lax.axis_size("rank")
    fits = (
        vpair_count == 4
        and rank_count == 8
        and amplitudes.shape[0] == 8
        and amplitudes.shape[1] == 2 * amplitudes.shape[2]
        and kernel.shape[1] % (128 * vpair_count) == 0
    )
    body = fast_shards if fits else shards
    return body(amplitudes, factors, kernel, other_terms, virt_energy, pair_energy)


def solution(mesh):
    placed = (
        P(None, "vpair", "rank"),
        P("vpair", "rank"),
        P("vpair", "rank"),
        P(None, "vpair", None),
        P(),
        P(),
    )
    return jax.shard_map(
        pick, mesh=mesh, in_specs=placed, out_specs=(P(None, "vpair", None), P()), check_vma=False
    )
```

```python
import functools

import jax
import jax.numpy as jnp
from jax import lax
from jax.experimental import pallas as pl
from jax.experimental.pallas import tpu as pltpu
from jax.sharding import PartitionSpec as P

epsilon = 1e-06


def shards(amplitudes, factors, kernel, other_terms, virt_energy, pair_energy):
    vpair_count = lax.axis_size("vpair")
    pair_count = amplitudes.shape[0]
    row_block = amplitudes.shape[1]
    col_block = amplitudes.shape[2]
    virt_count = row_block * vpair_count
    right_block = kernel.shape[1]
    factor_rows = lax.all_gather(factors, "rank", axis=1, tiled=True)
    factor_full = lax.all_gather(factor_rows, "vpair", axis=0, tiled=True)
    factor_cols = lax.dynamic_slice_in_dim(
        factor_full, lax.axis_index("rank") * right_block, right_block, 1
    )
    half_done = jnp.einsum(
        "ons,sh->onh",
        lax.all_gather(amplitudes, "rank", axis=2, tiled=True),
        factor_cols,
        preferred_element_type=jnp.float32,
    ).astype(jnp.bfloat16)
    kernel_sub = lax.all_to_all(kernel, "vpair", split_axis=1, concat_axis=0, tiled=True).astype(
        jnp.float32
    )
    coupled = jnp.einsum(
        "cp,icq->ipq",
        factor_full,
        lax.all_to_all(half_done, "vpair", split_axis=2, concat_axis=1, tiled=True),
        preferred_element_type=jnp.float32,
    )
    weighted = (kernel_sub[None] * coupled).astype(jnp.bfloat16)
    ladder_half = jnp.einsum(
        "ap,ipq->iaq", factor_full, weighted, preferred_element_type=jnp.float32
    ).astype(jnp.bfloat16)
    back_half = lax.all_to_all(ladder_half, "vpair", split_axis=1, concat_axis=2, tiled=True)
    partial_value = jnp.einsum(
        "iaq,bq->iab", back_half, factor_cols, preferred_element_type=jnp.float32
    )
    row_energy = lax.dynamic_slice_in_dim(
        virt_energy, lax.axis_index("vpair") * row_block, row_block, 0
    )
    ladder_share = lax.psum_scatter(partial_value, "rank", scatter_dimension=2, tiled=True)
    col_start = lax.axis_index("rank") * col_block
    own_terms = lax.dynamic_slice_in_dim(other_terms, col_start, col_block, 2)
    part_residual = own_terms + ladder_share
    col_energy = lax.dynamic_slice_in_dim(virt_energy, col_start, col_block, 0)
    denominator = row_energy[None, :, None] + col_energy[None, None, :] - pair_energy[:, None, None]
    update = part_residual / denominator
    squares = lax.psum(jnp.sum(update * update), ("vpair", "rank"))
    residual = lax.all_gather(part_residual, "rank", axis=2, tiled=True)
    update_rms = jnp.sqrt(squares / (pair_count * virt_count * virt_count) + epsilon)
    return (residual, update_rms)


MESH_IDS = pl.DeviceIdType.MESH


def middle_kernel(
    zs, cols_ref, line_ref, half_ref, kern_ref, early_ref, out_ref, fall, hrecv, hturn, kturn, late, acc,
    loc_sem, hr, fr, mr, xsend, msend, bs, br, far_sem, ks, kr,
):
    v = lax.axis_index("vpair")
    r = lax.axis_index("rank")
    y, x = v // 2, v % 2
    z, core = r // 2, r % 2
    vx, vy, vd = y * 2 + 1 - x, (1 - y) * 2 + x, (1 - y) * 2 + 1 - x
    near = (vx, vy, vd)
    mate = z * 2 + 1 - core
    pairs, count, block, cols = hrecv.shape
    depth = cols_ref.shape[2]
    rows = count * block
    group = 2
    groups = pairs // group
    tall = group * cols
    in_middle = jnp.logical_or(z == 1, z == 2)

    def line_at(k):
        return jnp.where(z < 2, (z + k) % zs, (z + zs - k) % zs)

    barrier = pltpu.get_barrier_semaphore()
    line_peers = [(v, ((z + k) % zs) * 2 + core) for k in (1, zs - 1)]
    peers = [(at, r) for at in near] + [(v, mate)] + line_peers
    for peer in peers:
        pl.semaphore_signal(barrier, inc=1, device_id=peer, device_id_type=MESH_IDS)
    pl.semaphore_wait(barrier, len(peers))

    def remote(src, dst, send_sem, recv_sem, to):
        return pltpu.make_async_remote_copy(
            src_ref=src, dst_ref=dst, send_sem=send_sem, recv_sem=recv_sem,
            device_id=to, device_id_type=MESH_IDS,
        )

    def own_half(i):
        return pltpu.make_async_copy(half_ref.at[i], hrecv.at[i], hr.at[i])

    def line_copy(k, slot):
        at = vd if slot else v
        rr = line_at(k) * 2 + core
        return pltpu.make_async_copy(line_ref.at[rr // 2, slot], fall.at[rr, at], fr.at[rr, at])

    def far_copy(slot):
        at = vd if slot else v
        far, to = jnp.where(z == 1, zs - 1, 0), jnp.where(z == 1, 0, zs - 1)
        rr = far * 2 + core
        return remote(
            line_ref.at[far, slot], fall.at[rr, at], far_sem.at[slot], fr.at[rr, at], (v, to * 2 + core)
        )

    def side_copy(k, j):
        rr = line_at(k) * 2 + core
        src = line_ref.at[rr // 2, 0] if k < zs - 1 else fall.at[rr, v]
        return remote(src, fall.at[rr, v], xsend.at[k, j], fr.at[rr, v], (near[j], r))

    def mate_copy(k):
        rr = line_at(k) * 2 + core
        return remote(fall.at[rr], fall.at[rr], msend.at[k], mr.at[rr], (v, mate))

    def shard_wait(rr, at):
        pltpu.make_async_copy(fall.at[rr, at], fall.at[rr, at], fr.at[rr, at]).wait()

    def late_part(at):
        side = pl.ds(pl.multiple_of((1 - core) * depth, depth), depth)
        return kern_ref.at[side, pl.ds(pl.multiple_of(at * cols, cols), cols)]

    def late_copy(j):
        return remote(late_part(near[j]), late.at[v], ks.at[j], kr.at[v], (near[j], r))

    def finish(k):
        rr = line_at(k) * 2 + core
        for at in (v, vx, vy, vd)[k == zs - 1 :]:
            shard_wait(rr, at)
        mate_copy(k).start()

    def spread_last():
        shard_wait(line_at(zs - 1) * 2 + core, v)
        for j in (0, 1):
            side_copy(zs - 1, j).start()
        for j in (0, 1, 2):
            late_copy(j).start()

    own_block = pltpu.make_async_copy(cols_ref, fall.at[r], loc_sem.at[0])
    mate_block = remote(cols_ref, fall.at[r], msend.at[0], mr.at[r], (v, mate))
    own_late = pltpu.make_async_copy(late_part(v), late.at[v], kr.at[v])
    own_block.start()
    for k in range(1, zs - 1):
        for j in (0, 1):
            side_copy(k, j).start()

    @pl.when(in_middle)
    def _():
        for slot in (0, 1):
            far_copy(slot).start()

    @pl.loop(0, pairs)
    def _(i):
        own_half(i).start()

    for k in range(1, zs - 1):
        for slot in (0, 1):
            line_copy(k, slot).start()

    @pl.when(in_middle)
    def _():
        for slot in (0, 1):
            line_copy(zs - 1, slot).start()

    mate_block.start()
    own_late.start()

    def compute(rr, slot, g):
        at = pl.multiple_of(g * tall, tall)
        shard = fall[rr].reshape(rows, depth)
        coupled = jnp.dot(hturn[pl.ds(at, tall), :], shard, preferred_element_type=jnp.float32)
        weight = kturn[slot].astype(jnp.float32)
        weighted = (coupled.reshape(group, cols, depth) * weight[None]).astype(jnp.bfloat16)
        return lax.dot_general(
            weighted.reshape(tall, depth), shard, (((1,), (1,)), ((), ())),
            preferred_element_type=jnp.float32,
        )

    kturn[0] = early_ref[z].T
    own_block.wait()

    @pl.loop(0, groups)
    def _(g):
        at = pl.multiple_of(g * tall, tall)
        for e in range(group):
            i = g * group + e
            own_half(i).wait()
            hturn[pl.ds(at + e * cols, cols), :] = hrecv[i].reshape(rows, cols).T
        acc[pl.ds(at, tall), :] = compute(r, 0, g)

    @pl.loop(1, zs)
    def _(k):
        for n in range(1, zs):

            @pl.when(k == n)
            def _():
                finish(n)
                if n == zs - 2:
                    spread_last()

        kturn[k] = early_ref[line_at(k)].T

        @pl.loop(0, groups)
        def _(g):
            at = pl.multiple_of(g * tall, tall)
            acc[pl.ds(at, tall), :] += compute(line_at(k) * 2 + core, k, g)

    def back_copy(i, j):
        return remote(hrecv.at[i, near[j]], out_ref.at[i, v], bs.at[i, j], br.at[i, v], (near[j], r))

    def own_back(i):
        return pltpu.make_async_copy(hrecv.at[i, v], out_ref.at[i, v], br.at[i, v])

    @pl.loop(0, groups)
    def _(g):
        at = pl.multiple_of(g * tall, tall)

        @pl.loop(0, count)
        def _(j):
            where = jnp.where(j < 2, jnp.where(j == 0, v, vx), jnp.where(j == 2, vy, vd))
            rr = where * 2 + 1 - core

            @pl.when(g == 0)
            def _():
                pltpu.make_async_copy(fall.at[rr], fall.at[rr], mr.at[rr]).wait()
                pltpu.make_async_copy(late.at[where], late.at[where], kr.at[where]).wait()
                kturn[j] = late[where].T

            acc[pl.ds(at, tall), :] += compute(rr, j, g)

        for e in range(group):
            i = g * group + e
            piece = acc[pl.ds(at + e * cols, cols), :].astype(jnp.bfloat16)
            hrecv[i] = piece.T.reshape(count, block, cols)
            for j in (0, 1, 2):
                back_copy(i, j).start()
            own_back(i).start()

    mate_block.wait_send()
    for k in range(1, zs):
        for j in (0, 1):
            side_copy(k, j).wait_send()
        mate_copy(k).wait_send()

    @pl.when(in_middle)
    def _():
        for slot in (0, 1):
            far_copy(slot).wait_send()

    for j in (0, 1, 2):
        late_copy(j).wait_send()

    @pl.loop(0, pairs)
    def _(i):
        for j in (0, 1, 2):
            back_copy(i, j).wait_send()
        for j in range(count):
            pltpu.make_async_copy(out_ref.at[i, j], out_ref.at[i, j], br.at[i, j]).wait()


def front_kernel(
    zs, col_block, own_ref, amp_ref, kern_ref, cols_ref, half_ref, z_ref, line_ref, turn_ref,
    cbuf, amps, zbuf, deep, hstage, tbuf,
    mine, cs, cr, us, ds, ms, ar, ks, kr, hs, hr, lu, ld, lr,
):
    v = lax.axis_index("vpair")
    r = lax.axis_index("rank")
    y, x = v // 2, v % 2
    z, core = r // 2, r % 2
    near = (y * 2 + 1 - x, (1 - y) * 2 + x, (1 - y) * 2 + 1 - x)
    vd = near[2]
    mate = z * 2 + 1 - core
    has_up, has_down = z + 1 < zs, z >= 1
    up_to, down_to = ((z + 1) % zs) * 2 + core, ((z + zs - 1) % zs) * 2 + core
    pairs, count, block, cols = half_ref.shape
    depth = own_ref.shape[1]
    rank_count, deep_block = amps.shape[:2]
    groups = hstage.shape[0]
    wide = hstage.shape[1]
    group = pairs // groups

    barrier = pltpu.get_barrier_semaphore()
    peers = [(at, r) for at in near] + [(v, mate), (v, up_to), (v, down_to)]
    for peer in peers:
        pl.semaphore_signal(barrier, inc=1, device_id=peer, device_id_type=MESH_IDS)
    pl.semaphore_wait(barrier, len(peers))

    def remote(src, dst, send_sem, recv_sem, to):
        return pltpu.make_async_remote_copy(
            src_ref=src, dst_ref=dst, send_sem=send_sem, recv_sem=recv_sem,
            device_id=to, device_id_type=MESH_IDS,
        )

    def arrive(ref, sem):
        pltpu.make_async_copy(ref, ref, sem).wait()

    def amps_copy(src, at, sem, to):
        return remote(src, amps.at[at], sem, ar.at[at], (v, to))

    def cols_copy(j):
        return remote(own_ref, cbuf.at[v], cs.at[j], cr.at[v], (near[j], r))

    def part_of(at):
        side = pl.ds(pl.multiple_of(core * depth, depth), depth)
        return kern_ref.at[side, pl.ds(pl.multiple_of(at * cols, cols), cols)]

    def kern_copy(j):
        return remote(part_of(near[j]), z_ref.at[v], ks.at[j], kr.at[v], (near[j], r))

    def line_copy(src, at, slot, sem, to):
        return remote(src, line_ref.at[at, slot], sem.at[at, slot], lr.at[at, slot], (v, to))

    def half_piece(i, at):
        rows_at = pl.multiple_of((i % group) * (wide // group), 16)
        return hstage.at[i // group, pl.ds(rows_at, block), pl.ds(pl.multiple_of(at * cols, cols), cols)]

    def half_copy(i, j):
        return remote(half_piece(i, near[j]), half_ref.at[i, v], hs.at[i, j], hr.at[i, v], (near[j], r))

    def own_half(i):
        return pltpu.make_async_copy(half_piece(i, v), half_ref.at[i, v], hr.at[i, v])

    @pl.when(has_up)
    def _():
        amps_copy(amp_ref, r, us.at[0], up_to).start()

    @pl.when(has_down)
    def _():
        amps_copy(amp_ref, r, ds.at[0], down_to).start()

    for j in (0, 1, 2):
        cols_copy(j).start()
    amps_copy(amp_ref, r, ms.at[0, 0], mate).start()
    for j in (0, 1, 2):
        kern_copy(j).start()
    own_cols = pltpu.make_async_copy(own_ref, cbuf.at[v], mine.at[0])
    own_amps = pltpu.make_async_copy(amp_ref, amps.at[r], mine.at[1])
    own_in = pltpu.make_async_copy(part_of(v), zbuf, mine.at[2])
    own_out = pltpu.make_async_copy(zbuf, z_ref.at[v], mine.at[2])
    own_cols.start()
    own_amps.start()
    own_in.start()
    deep[...] = jnp.zeros_like(deep)
    own_cols.wait()
    own_amps.wait()
    own_in.wait()
    own_out.start()

    def amps_step(s):
        low, high = ((z + zs - s) % zs) * 2 + core, ((z + s) % zs) * 2 + core

        @pl.when(z >= s)
        def _():
            arrive(amps.at[low], ar.at[low])
            amps_copy(amps.at[low], low, ms.at[s, 0], mate).start()

            @pl.when(has_up)
            def _():
                amps_copy(amps.at[low], low, us.at[s], up_to).start()

        @pl.when(z + s < zs)
        def _():
            arrive(amps.at[high], ar.at[high])
            amps_copy(amps.at[high], high, ms.at[s, 1], mate).start()

            @pl.when(has_down)
            def _():
                amps_copy(amps.at[high], high, ds.at[s], down_to).start()

    def line_step(s):
        low, high = (z + zs - s) % zs, (z + s) % zs

        @pl.when(z >= s)
        def _():
            for slot in (0, 1):
                arrive(line_ref.at[low, slot], lr.at[low, slot])

                if s < zs - 2:

                    @pl.when(has_up)
                    def _():
                        line_copy(line_ref.at[low, slot], low, slot, lu, up_to).start()

        @pl.when(z + s < zs)
        def _():
            for slot in (0, 1):
                arrive(line_ref.at[high, slot], lr.at[high, slot])

                if s < zs - 2:

                    @pl.when(has_down)
                    def _():
                        line_copy(line_ref.at[high, slot], high, slot, ld, down_to).start()

    for s in range(1, zs - 1):
        amps_step(s)
    for at in near:
        arrive(cbuf.at[at], cr.at[at])
    cols_out = pltpu.make_async_copy(cbuf, cols_ref, mine.at[0])
    cols_out.start()

    @pl.when(has_up)
    def _():
        for slot, at in ((0, v), (1, vd)):
            line_copy(cbuf.at[at], z, slot, lu, up_to).start()

    @pl.when(has_down)
    def _():
        for slot, at in ((0, v), (1, vd)):
            line_copy(cbuf.at[at], z, slot, ld, down_to).start()

    per = rank_count // count
    for j in range(count):
        whole = cbuf[j]
        for e in range(per):
            at = (j * per + e) * deep_block
            deep[at : at + col_block, :] = whole[e * col_block : (e + 1) * col_block]
    amps_step(zs - 1)
    for k in range(zs):
        at = k * 2 + 1 - core
        arrive(amps.at[at], ar.at[at])

    @pl.loop(0, groups)
    def _(g):
        left = amps[:, :, pl.ds(pl.multiple_of(g * wide, wide), wide)].reshape(rank_count * deep_block, wide)
        done = lax.dot_general(
            left, deep[...], (((0,), (0,)), ((), ())), preferred_element_type=jnp.float32
        )
        hstage[g] = done.astype(jnp.bfloat16)
        for e in range(group):
            i = g * group + e
            for j in (0, 1, 2):
                half_copy(i, j).start()
            own_half(i).start()

    flat = jnp.concatenate([cbuf[j, : per * col_block, :] for j in range(count)], axis=0)
    tbuf[...] = flat.T
    turn_out = pltpu.make_async_copy(tbuf, turn_ref, mine.at[1])
    turn_out.start()
    for s in range(1, zs - 1):
        line_step(s)
    for at in near:
        arrive(z_ref.at[at], kr.at[at])

    @pl.loop(0, pairs)
    def _(i):
        for j in range(count):
            arrive(half_ref.at[i, j], hr.at[i, j])
        for j in (0, 1, 2):
            half_copy(i, j).wait_send()

    own_out.wait()
    cols_out.wait()
    turn_out.wait()
    for j in (0, 1, 2):
        cols_copy(j).wait_send()
        kern_copy(j).wait_send()
    amps_copy(amp_ref, r, ms.at[0, 0], mate).wait_send()

    def line_sent(at, sem, to):
        for slot in (0, 1):
            line_copy(cbuf.at[0], at, slot, sem, to).wait_send()

    for s in range(zs):
        @pl.when(jnp.logical_and(z >= s, has_up))
        def _():
            amps_copy(amp_ref, r, us.at[s], up_to).wait_send()
            if s < zs - 2:
                line_sent((z + zs - s) % zs, lu, up_to)

        @pl.when(jnp.logical_and(z + s < zs, has_down))
        def _():
            amps_copy(amp_ref, r, ds.at[s], down_to).wait_send()
            if s < zs - 2:
                line_sent((z + s) % zs, ld, down_to)

        if s:

            @pl.when(z >= s)
            def _():
                amps_copy(amp_ref, r, ms.at[s, 0], mate).wait_send()

            @pl.when(z + s < zs)
            def _():
                amps_copy(amp_ref, r, ms.at[s, 1], mate).wait_send()


def front_gather(factors_pad, amps_pad, kernel, pairs, col_block, vpair_count, rank_count):
    zs = rank_count // 2
    block, right_block = factors_pad.shape
    cols = right_block // vpair_count
    deep_block, width = amps_pad.shape
    groups = pairs // 2
    hbm = pl.BlockSpec(memory_space=pl.ANY)
    dma = pltpu.SemaphoreType.DMA
    bf16 = lambda *shape: pltpu.VMEM(shape, jnp.bfloat16)
    like = lambda *shape: jax.ShapeDtypeStruct(shape, jnp.bfloat16)
    return pl.pallas_call(
        functools.partial(front_kernel, zs, col_block),
        out_shape=(
            like(vpair_count, block, right_block),
            like(pairs, vpair_count, block, cols),
            like(vpair_count, right_block, cols),
            like(zs, 2, block, right_block),
            like(right_block, rank_count * col_block),
        ),
        in_specs=[hbm, hbm, hbm],
        out_specs=(hbm, hbm, hbm, hbm, hbm),
        scratch_shapes=[
            bf16(vpair_count, block, right_block),
            bf16(rank_count, deep_block, width),
            bf16(right_block, cols),
            bf16(rank_count * deep_block, right_block),
            bf16(groups, width // groups, right_block),
            bf16(right_block, rank_count * col_block),
            dma((3,)),
            dma((3,)),
            dma((vpair_count,)),
            dma((zs,)),
            dma((zs,)),
            dma((zs, 2)),
            dma((rank_count,)),
            dma((3,)),
            dma((vpair_count,)),
            dma((pairs, 3)),
            dma((pairs, vpair_count)),
            dma((zs, 2)),
            dma((zs, 2)),
            dma((zs, 2)),
        ],
        compiler_params=pltpu.CompilerParams(
            collective_id=1, has_side_effects=True, vmem_limit_bytes=60 * 1024 * 1024
        ),
        cost_estimate=pl.CostEstimate(flops=10**10, bytes_accessed=10**7, transcendentals=0),
    )(factors_pad, amps_pad, kernel)


def ladder_middle(cols_pad, line, half, kernel, early, rank_count):
    count, block, depth = cols_pad.shape
    pairs = half.shape[0]
    cols = early.shape[2]
    rows = count * block
    points = rank_count * depth
    zs = rank_count // 2
    hbm = pl.BlockSpec(memory_space=pl.ANY)
    vmem = pl.BlockSpec(memory_space=pltpu.VMEM)
    dma = pltpu.SemaphoreType.DMA
    return pl.pallas_call(
        functools.partial(middle_kernel, zs),
        out_shape=jax.ShapeDtypeStruct((pairs, count, block, cols), jnp.bfloat16),
        in_specs=[hbm, hbm, hbm, hbm, vmem],
        out_specs=hbm,
        scratch_shapes=[
            pltpu.VMEM((rank_count, count, block, depth), jnp.bfloat16),
            pltpu.VMEM((pairs, count, block, cols), jnp.bfloat16),
            pltpu.VMEM((pairs * cols, rows), jnp.bfloat16),
            pltpu.VMEM((4, cols, depth), jnp.bfloat16),
            pltpu.VMEM((count, depth, cols), jnp.bfloat16),
            pltpu.VMEM((pairs * cols, rows), jnp.float32),
            dma((1,)),
            dma((pairs,)),
            dma((rank_count, count)),
            dma((rank_count,)),
            dma((zs, 2)),
            dma((zs,)),
            dma((pairs, 3)),
            dma((pairs, count)),
            dma((2,)),
            dma((3,)),
            dma((count,)),
        ],
        compiler_params=pltpu.CompilerParams(
            collective_id=0, has_side_effects=True, vmem_limit_bytes=62 * 1024 * 1024
        ),
        cost_estimate=pl.CostEstimate(
            flops=4 * pairs * points * rows * cols, bytes_accessed=4 * points * rows, transcendentals=0
        ),
    )(cols_pad, line, half, kernel, early)


CUTS = 4


def tail_kernel(
    back_ref, turned, other_ref, rowen_ref, virt_ref, res_ref, sq_ref,
    part, msend, mrecv, zsend, outer, inner, fin, oth, sq, sqall,
    ms, mr, zs_sem, outr, inr, fs, fr, osem, rsem, qs, qr,
):
    v = lax.axis_index("vpair")
    r = lax.axis_index("rank")
    y, x = v // 2, v % 2
    z, core = r // 2, r % 2
    near = (y * 2 + 1 - x, (1 - y) * 2 + x, (1 - y) * 2 + 1 - x)
    mate = z * 2 + 1 - core
    pairs, count, block, cols = back_ref.shape
    rows = part.shape[1]
    turns = pairs // 2
    step_rows = -(-rows // (16 * CUTS)) * 16
    cuts = [(h * step_rows, min(step_rows, rows - h * step_rows)) for h in range(CUTS)]
    at_end = jnp.logical_or(z == 0, z == 3)
    in_middle = jnp.logical_not(at_end)
    toward_at = (v, jnp.where(z < 2, z + 1, z - 1) * 2 + core)
    away_at = (v, jnp.where(z == 1, 0, 3) * 2 + core)
    mate_at = (v, mate)

    barrier = pltpu.get_barrier_semaphore()
    for peer in [(at, r) for at in near] + [mate_at, toward_at]:
        pl.semaphore_signal(barrier, inc=1, device_id=peer, device_id_type=MESH_IDS)

    @pl.when(in_middle)
    def _():
        pl.semaphore_signal(barrier, inc=1, device_id=away_at, device_id_type=MESH_IDS)
        pl.semaphore_wait(barrier, 6)

    @pl.when(at_end)
    def _():
        pl.semaphore_wait(barrier, 5)

    def remote(src, dst, send_sem, recv_sem, to):
        return pltpu.make_async_remote_copy(
            src_ref=src, dst_ref=dst, send_sem=send_sem, recv_sem=recv_sem,
            device_id=to, device_id_type=MESH_IDS,
        )

    def arrive(ref, sem):
        pltpu.make_async_copy(ref, ref, sem).wait()

    def other_copy(p):
        return pltpu.make_async_copy(other_ref.at[:, p], oth.at[p], osem.at[p])

    def cut(ref, t, h):
        return ref.at[t, pl.ds(*cuts[h]), :]

    def read(ref, t, h):
        return ref[t, pl.ds(*cuts[h]), :].astype(jnp.float32)

    def res_copy(p, h):
        return pltpu.make_async_copy(cut(oth, p, h), res_ref.at[pl.ds(*cuts[h]), p], rsem.at[p, h])

    def mate_copy(t):
        return remote(msend.at[t], mrecv.at[t], ms.at[t], mr.at[t], mate_at)

    def outer_copy(t, h):
        return remote(cut(zsend, t, h), cut(outer, t, h), zs_sem.at[t, h], outr.at[t, h], toward_at)

    def inner_copy(t, h):
        return remote(cut(zsend, t, h), cut(inner, t, h), zs_sem.at[t, h], inr.at[t, h], toward_at)

    def fin_copy(p, h, j, to):
        return remote(cut(fin, p, h), cut(fin, p, h), fs.at[p // 2, h, j], fr.at[p, h], to)

    def ladder(p):
        left = jnp.concatenate([back_ref[p, j] for j in range(count)], axis=1)
        return jnp.dot(left, turned[...], preferred_element_type=jnp.float32)[:rows]

    def make(t):
        msend[t] = ladder(2 * t + 1 - core).astype(jnp.bfloat16)
        mate_copy(t).start()
        part[t] = ladder(2 * t + core)

    def give(t, h):
        if h == 0:
            arrive(mrecv.at[t], mr.at[t])

        @pl.when(at_end)
        def _():
            zsend[t, pl.ds(*cuts[h]), :] = (read(part, t, h) + read(mrecv, t, h)).astype(jnp.bfloat16)
            outer_copy(t, h).start()

    def meet(t, h):
        @pl.when(in_middle)
        def _():
            arrive(cut(outer, t, h), outr.at[t, h])
            both = read(part, t, h) + read(mrecv, t, h)
            zsend[t, pl.ds(*cuts[h]), :] = (both + read(outer, t, h)).astype(jnp.bfloat16)
            inner_copy(t, h).start()

    def close(t, h):
        p = 2 * t + core

        @pl.when(in_middle)
        def _():
            arrive(cut(inner, t, h), inr.at[t, h])
            fin[p, pl.ds(*cuts[h]), :] = (read(zsend, t, h) + read(inner, t, h)).astype(jnp.bfloat16)
            fin_copy(p, h, 0, away_at).start()
            fin_copy(p, h, 1, mate_at).start()

    def land(t, h):
        p = 2 * t + core

        @pl.when(at_end)
        def _():
            arrive(cut(fin, p, h), fr.at[p, h])
            fin_copy(p, h, 1, mate_at).start()

    def settle(t, h):
        q = 2 * t + 1 - core
        arrive(cut(fin, q, h), fr.at[q, h])
        for e in range(2):
            p = 2 * t + e
            if h == 0:
                other_copy(p).wait()
            value = read(oth, p, h) + read(fin, p, h)
            oth[p, pl.ds(*cuts[h]), :] = value
            update = value / (rowen_ref[p, pl.ds(*cuts[h]), :] + virt_ref[...])
            squares = jnp.sum(update * update, axis=0, keepdims=True)
            if h == 0:
                sq[pl.ds(p, 1), :] = squares
            else:
                sq[pl.ds(p, 1), :] += squares
            res_copy(p, h).start()

    @pl.loop(0, pairs)
    def _(p):
        other_copy(p).start()

    stages = ((1, give), (3, meet), (5, close), (7, land), (8, settle))
    last = stages[-1][0]

    @pl.loop(0, turns + -(-last // CUTS))
    def _(u):
        @pl.when(u < turns)
        def _():
            make(u)

        for h in range(CUTS):
            for lag, stage in stages:
                t = u + (h - lag) // CUTS

                @pl.when(jnp.logical_and(t >= 0, t < turns))
                def _():
                    stage(t, (h - lag) % CUTS)

    sqall[v] = sq[...]
    for j in range(3):
        remote(sq, sqall.at[v], qs.at[j], qr.at[v], (near[j], r)).start()
    for at in near:
        arrive(sqall.at[at], qr.at[at])
    total = (sqall[0] + sqall[1]) + (sqall[2] + sqall[3])
    sq_ref[...] = jnp.sum(jnp.sum(total, axis=1, keepdims=True), axis=0, keepdims=True)

    for j in range(3):
        remote(sq, sqall.at[v], qs.at[j], qr.at[v], (near[j], r)).wait_send()

    @pl.loop(0, turns)
    def _(t):
        mate_copy(t).wait_send()
        for h in range(CUTS):
            outer_copy(t, h).wait_send()
            fin_copy(2 * t + core, h, 1, mate_at).wait_send()

            @pl.when(in_middle)
            def _():
                fin_copy(2 * t + core, h, 0, away_at).wait_send()

            for e in range(2):
                res_copy(2 * t + e, h).wait()


def ladder_tail(back, turned, other_turned, row_energy, virt_energy):
    pairs, count, block, cols = back.shape
    rows = other_turned.shape[0]
    depth, virt_count = turned.shape
    turns = pairs // 2
    hbm = pl.BlockSpec(memory_space=pl.ANY)
    vmem = pl.BlockSpec(memory_space=pltpu.VMEM)
    dma = pltpu.SemaphoreType.DMA
    bf16 = lambda *shape: pltpu.VMEM(shape, jnp.bfloat16)
    f32 = lambda *shape: pltpu.VMEM(shape, jnp.float32)
    return pl.pallas_call(
        tail_kernel,
        out_shape=(
            jax.ShapeDtypeStruct((rows, pairs, virt_count), jnp.float32),
            jax.ShapeDtypeStruct((1, 1), jnp.float32),
        ),
        in_specs=[vmem, vmem, hbm, vmem, vmem],
        out_specs=(hbm, vmem),
        scratch_shapes=[
            f32(turns, rows, virt_count),
            bf16(turns, rows, virt_count),
            bf16(turns, rows, virt_count),
            bf16(turns, rows, virt_count),
            bf16(turns, rows, virt_count),
            bf16(turns, rows, virt_count),
            bf16(pairs, rows, virt_count),
            f32(pairs, rows, virt_count),
            f32(pairs, virt_count),
            f32(count, pairs, virt_count),
            dma((turns,)),
            dma((turns,)),
            dma((turns, CUTS)),
            dma((turns, CUTS)),
            dma((turns, CUTS)),
            dma((turns, CUTS, 2)),
            dma((pairs, CUTS)),
            dma((pairs,)),
            dma((pairs, CUTS)),
            dma((3,)),
            dma((count,)),
        ],
        compiler_params=pltpu.CompilerParams(
            collective_id=2, has_side_effects=True, vmem_limit_bytes=62 * 1024 * 1024
        ),
        cost_estimate=pl.CostEstimate(
            flops=2 * pairs * rows * virt_count * depth, bytes_accessed=8 * pairs * rows * virt_count,
            transcendentals=0,
        ),
    )(back, turned, other_turned, row_energy, virt_energy)


def fast_shards(amplitudes, factors, kernel, other_terms, virt_energy, pair_energy):
    vpair_count = lax.axis_size("vpair")
    rank_count = lax.axis_size("rank")
    pair_count, row_block, _ = amplitudes.shape
    virt_count = row_block * vpair_count
    block = -(-row_block // 16) * 16
    tall = -(-row_block // 64) * 64
    col_block = amplitudes.shape[2]
    deep = -(-col_block // 16) * 16
    factors_pad = jnp.pad(factors, ((0, block - row_block), (0, 0)))
    amps_pad = jnp.pad(
        amplitudes.transpose(2, 0, 1), ((0, deep - col_block), (0, 0), (0, tall - row_block))
    ).reshape(deep, pair_count * tall)
    cols_pad, half, early, line, turned = front_gather(
        factors_pad, amps_pad, kernel, pair_count, col_block, vpair_count, rank_count
    )
    back = ladder_middle(cols_pad, line, half, kernel, early, rank_count)
    row_energy = lax.dynamic_slice_in_dim(
        virt_energy, lax.axis_index("vpair") * row_block, row_block, 0
    )
    shifted = row_energy[None, :, None] - pair_energy[:, None, None]
    residual, squares = ladder_tail(
        back, turned, other_terms.transpose(1, 0, 2), shifted, virt_energy[None, :]
    )
    update_rms = jnp.sqrt(squares[0, 0] / (pair_count * virt_count * virt_count) + epsilon)
    return (residual.transpose(1, 0, 2), update_rms)


def pick(amplitudes, factors, kernel, other_terms, virt_energy, pair_energy):
    vpair_count = lax.axis_size("vpair")
    rank_count = lax.axis_size("rank")
    fits = (
        vpair_count == 4
        and rank_count == 8
        and amplitudes.shape[0] == 8
        and amplitudes.shape[1] == 2 * amplitudes.shape[2]
        and kernel.shape[1] % (128 * vpair_count) == 0
    )
    body = fast_shards if fits else shards
    return body(amplitudes, factors, kernel, other_terms, virt_energy, pair_energy)


def solution(mesh):
    placed = (
        P(None, "vpair", "rank"),
        P("vpair", "rank"),
        P("vpair", "rank"),
        P(None, "vpair", None),
        P(),
        P(),
    )
    return jax.shard_map(
        pick, mesh=mesh, in_specs=placed, out_specs=(P(None, "vpair", None), P()), check_vma=False
    )
```

```python
import functools

import jax
import jax.numpy as jnp
from jax import lax
from jax.experimental import pallas as pl
from jax.experimental.pallas import tpu as pltpu
from jax.sharding import PartitionSpec as P

epsilon = 1e-06


def shards(amplitudes, factors, kernel, other_terms, virt_energy, pair_energy):
    vpair_count = lax.axis_size("vpair")
    pair_count = amplitudes.shape[0]
    row_block = amplitudes.shape[1]
    col_block = amplitudes.shape[2]
    virt_count = row_block * vpair_count
    right_block = kernel.shape[1]
    factor_rows = lax.all_gather(factors, "rank", axis=1, tiled=True)
    factor_full = lax.all_gather(factor_rows, "vpair", axis=0, tiled=True)
    factor_cols = lax.dynamic_slice_in_dim(
        factor_full, lax.axis_index("rank") * right_block, right_block, 1
    )
    half_done = jnp.einsum(
        "ons,sh->onh",
        lax.all_gather(amplitudes, "rank", axis=2, tiled=True),
        factor_cols,
        preferred_element_type=jnp.float32,
    ).astype(jnp.bfloat16)
    kernel_sub = lax.all_to_all(kernel, "vpair", split_axis=1, concat_axis=0, tiled=True).astype(
        jnp.float32
    )
    coupled = jnp.einsum(
        "cp,icq->ipq",
        factor_full,
        lax.all_to_all(half_done, "vpair", split_axis=2, concat_axis=1, tiled=True),
        preferred_element_type=jnp.float32,
    )
    weighted = (kernel_sub[None] * coupled).astype(jnp.bfloat16)
    ladder_half = jnp.einsum(
        "ap,ipq->iaq", factor_full, weighted, preferred_element_type=jnp.float32
    ).astype(jnp.bfloat16)
    back_half = lax.all_to_all(ladder_half, "vpair", split_axis=1, concat_axis=2, tiled=True)
    partial_value = jnp.einsum(
        "iaq,bq->iab", back_half, factor_cols, preferred_element_type=jnp.float32
    )
    row_energy = lax.dynamic_slice_in_dim(
        virt_energy, lax.axis_index("vpair") * row_block, row_block, 0
    )
    ladder_share = lax.psum_scatter(partial_value, "rank", scatter_dimension=2, tiled=True)
    col_start = lax.axis_index("rank") * col_block
    own_terms = lax.dynamic_slice_in_dim(other_terms, col_start, col_block, 2)
    part_residual = own_terms + ladder_share
    col_energy = lax.dynamic_slice_in_dim(virt_energy, col_start, col_block, 0)
    denominator = row_energy[None, :, None] + col_energy[None, None, :] - pair_energy[:, None, None]
    update = part_residual / denominator
    squares = lax.psum(jnp.sum(update * update), ("vpair", "rank"))
    residual = lax.all_gather(part_residual, "rank", axis=2, tiled=True)
    update_rms = jnp.sqrt(squares / (pair_count * virt_count * virt_count) + epsilon)
    return (residual, update_rms)


MESH_IDS = pl.DeviceIdType.MESH


def middle_kernel(
    zs, cols_ref, line_ref, half_ref, kern_ref, early_ref, out_ref, fall, hrecv, hturn, kturn, late, acc,
    loc_sem, hr, fr, mr, xsend, msend, bs, br, far_sem, ks, kr,
):
    v = lax.axis_index("vpair")
    r = lax.axis_index("rank")
    y, x = v // 2, v % 2
    z, core = r // 2, r % 2
    vx, vy, vd = y * 2 + 1 - x, (1 - y) * 2 + x, (1 - y) * 2 + 1 - x
    near = (vx, vy, vd)
    mate = z * 2 + 1 - core
    pairs, count, block, cols = hrecv.shape
    depth = cols_ref.shape[2]
    rows = count * block
    group = 2
    groups = pairs // group
    tall = group * cols
    in_middle = jnp.logical_or(z == 1, z == 2)

    def line_at(k):
        return jnp.where(z < 2, (z + k) % zs, (z + zs - k) % zs)

    barrier = pltpu.get_barrier_semaphore()
    line_peers = [(v, ((z + k) % zs) * 2 + core) for k in (1, zs - 1)]
    peers = [(at, r) for at in near] + [(v, mate)] + line_peers
    for peer in peers:
        pl.semaphore_signal(barrier, inc=1, device_id=peer, device_id_type=MESH_IDS)
    pl.semaphore_wait(barrier, len(peers))

    def remote(src, dst, send_sem, recv_sem, to):
        return pltpu.make_async_remote_copy(
            src_ref=src, dst_ref=dst, send_sem=send_sem, recv_sem=recv_sem,
            device_id=to, device_id_type=MESH_IDS,
        )

    def own_half(i):
        return pltpu.make_async_copy(half_ref.at[i], hrecv.at[i], hr.at[i])

    def line_copy(k, slot):
        at = vd if slot else v
        rr = line_at(k) * 2 + core
        return pltpu.make_async_copy(line_ref.at[rr // 2, slot], fall.at[rr, at], fr.at[rr, at])

    def far_copy(slot):
        at = vd if slot else v
        far, to = jnp.where(z == 1, zs - 1, 0), jnp.where(z == 1, 0, zs - 1)
        rr = far * 2 + core
        return remote(
            line_ref.at[far, slot], fall.at[rr, at], far_sem.at[slot], fr.at[rr, at], (v, to * 2 + core)
        )

    def side_copy(k, j):
        rr = line_at(k) * 2 + core
        src = line_ref.at[rr // 2, 0] if k < zs - 1 else fall.at[rr, v]
        return remote(src, fall.at[rr, v], xsend.at[k, j], fr.at[rr, v], (near[j], r))

    def mate_copy(k):
        rr = line_at(k) * 2 + core
        return remote(fall.at[rr], fall.at[rr], msend.at[k], mr.at[rr], (v, mate))

    def shard_wait(rr, at):
        pltpu.make_async_copy(fall.at[rr, at], fall.at[rr, at], fr.at[rr, at]).wait()

    def late_part(at):
        side = pl.ds(pl.multiple_of((1 - core) * depth, depth), depth)
        return kern_ref.at[side, pl.ds(pl.multiple_of(at * cols, cols), cols)]

    def late_copy(j):
        return remote(late_part(near[j]), late.at[v], ks.at[j], kr.at[v], (near[j], r))

    def finish(k):
        rr = line_at(k) * 2 + core
        for at in (v, vx, vy, vd)[k == zs - 1 :]:
            shard_wait(rr, at)
        mate_copy(k).start()

    def spread_last():
        shard_wait(line_at(zs - 1) * 2 + core, v)
        for j in (0, 1):
            side_copy(zs - 1, j).start()
        for j in (0, 1, 2):
            late_copy(j).start()

    own_block = pltpu.make_async_copy(cols_ref, fall.at[r], loc_sem.at[0])
    mate_block = remote(cols_ref, fall.at[r], msend.at[0], mr.at[r], (v, mate))
    own_late = pltpu.make_async_copy(late_part(v), late.at[v], kr.at[v])
    own_block.start()
    for k in range(1, zs - 1):
        for j in (0, 1):
            side_copy(k, j).start()

    @pl.when(in_middle)
    def _():
        for slot in (0, 1):
            far_copy(slot).start()

    @pl.loop(0, pairs)
    def _(i):
        own_half(i).start()

    for k in range(1, zs - 1):
        for slot in (0, 1):
            line_copy(k, slot).start()

    @pl.when(in_middle)
    def _():
        for slot in (0, 1):
            line_copy(zs - 1, slot).start()

    mate_block.start()
    own_late.start()

    def compute(rr, slot, g):
        at = pl.multiple_of(g * tall, tall)
        shard = fall[rr].reshape(rows, depth)
        coupled = jnp.dot(hturn[pl.ds(at, tall), :], shard, preferred_element_type=jnp.float32)
        weight = kturn[slot].astype(jnp.float32)
        weighted = (coupled.reshape(group, cols, depth) * weight[None]).astype(jnp.bfloat16)
        return lax.dot_general(
            weighted.reshape(tall, depth), shard, (((1,), (1,)), ((), ())),
            preferred_element_type=jnp.float32,
        )

    kturn[0] = early_ref[z].T
    own_block.wait()

    @pl.loop(0, groups)
    def _(g):
        at = pl.multiple_of(g * tall, tall)
        for e in range(group):
            i = g * group + e
            own_half(i).wait()
            hturn[pl.ds(at + e * cols, cols), :] = hrecv[i].reshape(rows, cols).T
        acc[pl.ds(at, tall), :] = compute(r, 0, g)

    @pl.loop(1, zs)
    def _(k):
        for n in range(1, zs):

            @pl.when(k == n)
            def _():
                finish(n)
                if n == zs - 2:
                    spread_last()

        kturn[k] = early_ref[line_at(k)].T

        @pl.loop(0, groups)
        def _(g):
            at = pl.multiple_of(g * tall, tall)
            acc[pl.ds(at, tall), :] += compute(line_at(k) * 2 + core, k, g)

    def back_copy(i, j):
        return remote(hrecv.at[i, near[j]], out_ref.at[i, v], bs.at[i, j], br.at[i, v], (near[j], r))

    def own_back(i):
        return pltpu.make_async_copy(hrecv.at[i, v], out_ref.at[i, v], br.at[i, v])

    @pl.loop(0, groups)
    def _(g):
        at = pl.multiple_of(g * tall, tall)

        @pl.loop(0, count)
        def _(j):
            where = jnp.where(j < 2, jnp.where(j == 0, v, vx), jnp.where(j == 2, vy, vd))
            rr = where * 2 + 1 - core

            @pl.when(g == 0)
            def _():
                pltpu.make_async_copy(fall.at[rr], fall.at[rr], mr.at[rr]).wait()
                pltpu.make_async_copy(late.at[where], late.at[where], kr.at[where]).wait()
                kturn[j] = late[where].T

            acc[pl.ds(at, tall), :] += compute(rr, j, g)

        for e in range(group):
            i = g * group + e
            piece = acc[pl.ds(at + e * cols, cols), :].astype(jnp.bfloat16)
            hrecv[i] = piece.T.reshape(count, block, cols)
            for j in (0, 1, 2):
                back_copy(i, j).start()
            own_back(i).start()

    mate_block.wait_send()
    for k in range(1, zs):
        for j in (0, 1):
            side_copy(k, j).wait_send()
        mate_copy(k).wait_send()

    @pl.when(in_middle)
    def _():
        for slot in (0, 1):
            far_copy(slot).wait_send()

    for j in (0, 1, 2):
        late_copy(j).wait_send()

    @pl.loop(0, pairs)
    def _(i):
        for j in (0, 1, 2):
            back_copy(i, j).wait_send()
        for j in range(count):
            pltpu.make_async_copy(out_ref.at[i, j], out_ref.at[i, j], br.at[i, j]).wait()


def front_kernel(
    zs, col_block, own_ref, amp_ref, kern_ref, cols_ref, half_ref, z_ref, line_ref, turn_ref,
    cbuf, amps, zbuf, deep, hstage, tbuf,
    mine, cs, cr, us, ds, ms, ar, ks, kr, hs, hr, lu, ld, lr,
):
    v = lax.axis_index("vpair")
    r = lax.axis_index("rank")
    y, x = v // 2, v % 2
    z, core = r // 2, r % 2
    near = (y * 2 + 1 - x, (1 - y) * 2 + x, (1 - y) * 2 + 1 - x)
    vd = near[2]
    mate = z * 2 + 1 - core
    has_up, has_down = z + 1 < zs, z >= 1
    up_to, down_to = ((z + 1) % zs) * 2 + core, ((z + zs - 1) % zs) * 2 + core
    pairs, count, block, cols = half_ref.shape
    depth = own_ref.shape[1]
    rank_count, deep_block = amps.shape[:2]
    groups = hstage.shape[0]
    wide = hstage.shape[1]
    group = pairs // groups

    barrier = pltpu.get_barrier_semaphore()
    peers = [(at, r) for at in near] + [(v, mate), (v, up_to), (v, down_to)]
    for peer in peers:
        pl.semaphore_signal(barrier, inc=1, device_id=peer, device_id_type=MESH_IDS)
    pl.semaphore_wait(barrier, len(peers))

    def remote(src, dst, send_sem, recv_sem, to):
        return pltpu.make_async_remote_copy(
            src_ref=src, dst_ref=dst, send_sem=send_sem, recv_sem=recv_sem,
            device_id=to, device_id_type=MESH_IDS,
        )

    def arrive(ref, sem):
        pltpu.make_async_copy(ref, ref, sem).wait()

    def amps_copy(src, at, sem, to):
        return remote(src, amps.at[at], sem, ar.at[at], (v, to))

    def cols_copy(j):
        return remote(own_ref, cbuf.at[v], cs.at[j], cr.at[v], (near[j], r))

    def part_of(at):
        side = pl.ds(pl.multiple_of(core * depth, depth), depth)
        return kern_ref.at[side, pl.ds(pl.multiple_of(at * cols, cols), cols)]

    def kern_copy(j):
        return remote(part_of(near[j]), z_ref.at[v], ks.at[j], kr.at[v], (near[j], r))

    def line_copy(src, at, slot, sem, to):
        return remote(src, line_ref.at[at, slot], sem.at[at, slot], lr.at[at, slot], (v, to))

    def half_piece(i, at):
        rows_at = pl.multiple_of((i % group) * (wide // group), 16)
        return hstage.at[i // group, pl.ds(rows_at, block), pl.ds(pl.multiple_of(at * cols, cols), cols)]

    def half_copy(i, j):
        return remote(half_piece(i, near[j]), half_ref.at[i, v], hs.at[i, j], hr.at[i, v], (near[j], r))

    def own_half(i):
        return pltpu.make_async_copy(half_piece(i, v), half_ref.at[i, v], hr.at[i, v])

    @pl.when(has_up)
    def _():
        amps_copy(amp_ref, r, us.at[0], up_to).start()

    @pl.when(has_down)
    def _():
        amps_copy(amp_ref, r, ds.at[0], down_to).start()

    for j in (0, 1, 2):
        cols_copy(j).start()
    amps_copy(amp_ref, r, ms.at[0, 0], mate).start()
    for j in (0, 1, 2):
        kern_copy(j).start()
    own_cols = pltpu.make_async_copy(own_ref, cbuf.at[v], mine.at[0])
    own_amps = pltpu.make_async_copy(amp_ref, amps.at[r], mine.at[1])
    own_in = pltpu.make_async_copy(part_of(v), zbuf, mine.at[2])
    own_out = pltpu.make_async_copy(zbuf, z_ref.at[v], mine.at[2])
    own_cols.start()
    own_amps.start()
    own_in.start()
    deep[...] = jnp.zeros_like(deep)
    own_cols.wait()
    own_amps.wait()
    own_in.wait()
    own_out.start()

    def amps_step(s):
        low, high = ((z + zs - s) % zs) * 2 + core, ((z + s) % zs) * 2 + core

        @pl.when(z >= s)
        def _():
            arrive(amps.at[low], ar.at[low])
            amps_copy(amps.at[low], low, ms.at[s, 0], mate).start()

            @pl.when(has_up)
            def _():
                amps_copy(amps.at[low], low, us.at[s], up_to).start()

        @pl.when(z + s < zs)
        def _():
            arrive(amps.at[high], ar.at[high])
            amps_copy(amps.at[high], high, ms.at[s, 1], mate).start()

            @pl.when(has_down)
            def _():
                amps_copy(amps.at[high], high, ds.at[s], down_to).start()

    def line_step(s):
        low, high = (z + zs - s) % zs, (z + s) % zs

        @pl.when(z >= s)
        def _():
            for slot in (0, 1):
                arrive(line_ref.at[low, slot], lr.at[low, slot])

                if s < zs - 2:

                    @pl.when(has_up)
                    def _():
                        line_copy(line_ref.at[low, slot], low, slot, lu, up_to).start()

        @pl.when(z + s < zs)
        def _():
            for slot in (0, 1):
                arrive(line_ref.at[high, slot], lr.at[high, slot])

                if s < zs - 2:

                    @pl.when(has_down)
                    def _():
                        line_copy(line_ref.at[high, slot], high, slot, ld, down_to).start()

    for s in range(1, zs - 1):
        amps_step(s)
    for at in near:
        arrive(cbuf.at[at], cr.at[at])
    cols_out = pltpu.make_async_copy(cbuf, cols_ref, mine.at[0])
    cols_out.start()

    @pl.when(has_up)
    def _():
        for slot, at in ((0, v), (1, vd)):
            line_copy(cbuf.at[at], z, slot, lu, up_to).start()

    @pl.when(has_down)
    def _():
        for slot, at in ((0, v), (1, vd)):
            line_copy(cbuf.at[at], z, slot, ld, down_to).start()

    per = rank_count // count
    for j in range(count):
        whole = cbuf[j]
        for e in range(per):
            at = (j * per + e) * deep_block
            deep[at : at + col_block, :] = whole[e * col_block : (e + 1) * col_block]
    amps_step(zs - 1)
    for k in range(zs):
        at = k * 2 + 1 - core
        arrive(amps.at[at], ar.at[at])

    @pl.loop(0, groups)
    def _(g):
        left = amps[:, :, pl.ds(pl.multiple_of(g * wide, wide), wide)].reshape(rank_count * deep_block, wide)
        done = lax.dot_general(
            left, deep[...], (((0,), (0,)), ((), ())), preferred_element_type=jnp.float32
        )
        hstage[g] = done.astype(jnp.bfloat16)
        for e in range(group):
            i = g * group + e
            for j in (0, 1, 2):
                half_copy(i, j).start()
            own_half(i).start()

    flat = jnp.concatenate([cbuf[j, : per * col_block, :] for j in range(count)], axis=0)
    tbuf[...] = flat.T
    turn_out = pltpu.make_async_copy(tbuf, turn_ref, mine.at[1])
    turn_out.start()
    for s in range(1, zs - 1):
        line_step(s)
    for at in near:
        arrive(z_ref.at[at], kr.at[at])

    @pl.loop(0, pairs)
    def _(i):
        for j in range(count):
            arrive(half_ref.at[i, j], hr.at[i, j])
        for j in (0, 1, 2):
            half_copy(i, j).wait_send()

    own_out.wait()
    cols_out.wait()
    turn_out.wait()
    for j in (0, 1, 2):
        cols_copy(j).wait_send()
        kern_copy(j).wait_send()
    amps_copy(amp_ref, r, ms.at[0, 0], mate).wait_send()

    def line_sent(at, sem, to):
        for slot in (0, 1):
            line_copy(cbuf.at[0], at, slot, sem, to).wait_send()

    for s in range(zs):
        @pl.when(jnp.logical_and(z >= s, has_up))
        def _():
            amps_copy(amp_ref, r, us.at[s], up_to).wait_send()
            if s < zs - 2:
                line_sent((z + zs - s) % zs, lu, up_to)

        @pl.when(jnp.logical_and(z + s < zs, has_down))
        def _():
            amps_copy(amp_ref, r, ds.at[s], down_to).wait_send()
            if s < zs - 2:
                line_sent((z + s) % zs, ld, down_to)

        if s:

            @pl.when(z >= s)
            def _():
                amps_copy(amp_ref, r, ms.at[s, 0], mate).wait_send()

            @pl.when(z + s < zs)
            def _():
                amps_copy(amp_ref, r, ms.at[s, 1], mate).wait_send()


def front_gather(factors_pad, amps_pad, kernel, pairs, col_block, vpair_count, rank_count):
    zs = rank_count // 2
    block, right_block = factors_pad.shape
    cols = right_block // vpair_count
    deep_block, width = amps_pad.shape
    groups = pairs // 2
    hbm = pl.BlockSpec(memory_space=pl.ANY)
    dma = pltpu.SemaphoreType.DMA
    bf16 = lambda *shape: pltpu.VMEM(shape, jnp.bfloat16)
    like = lambda *shape: jax.ShapeDtypeStruct(shape, jnp.bfloat16)
    return pl.pallas_call(
        functools.partial(front_kernel, zs, col_block),
        out_shape=(
            like(vpair_count, block, right_block),
            like(pairs, vpair_count, block, cols),
            like(vpair_count, right_block, cols),
            like(zs, 2, block, right_block),
            like(right_block, rank_count * col_block),
        ),
        in_specs=[hbm, hbm, hbm],
        out_specs=(hbm, hbm, hbm, hbm, hbm),
        scratch_shapes=[
            bf16(vpair_count, block, right_block),
            bf16(rank_count, deep_block, width),
            bf16(right_block, cols),
            bf16(rank_count * deep_block, right_block),
            bf16(groups, width // groups, right_block),
            bf16(right_block, rank_count * col_block),
            dma((3,)),
            dma((3,)),
            dma((vpair_count,)),
            dma((zs,)),
            dma((zs,)),
            dma((zs, 2)),
            dma((rank_count,)),
            dma((3,)),
            dma((vpair_count,)),
            dma((pairs, 3)),
            dma((pairs, vpair_count)),
            dma((zs, 2)),
            dma((zs, 2)),
            dma((zs, 2)),
        ],
        compiler_params=pltpu.CompilerParams(
            collective_id=1, has_side_effects=True, vmem_limit_bytes=60 * 1024 * 1024
        ),
        cost_estimate=pl.CostEstimate(flops=10**10, bytes_accessed=10**7, transcendentals=0),
    )(factors_pad, amps_pad, kernel)


def ladder_middle(cols_pad, line, half, kernel, early, rank_count):
    count, block, depth = cols_pad.shape
    pairs = half.shape[0]
    cols = early.shape[2]
    rows = count * block
    points = rank_count * depth
    zs = rank_count // 2
    hbm = pl.BlockSpec(memory_space=pl.ANY)
    vmem = pl.BlockSpec(memory_space=pltpu.VMEM)
    dma = pltpu.SemaphoreType.DMA
    return pl.pallas_call(
        functools.partial(middle_kernel, zs),
        out_shape=jax.ShapeDtypeStruct((pairs, count, block, cols), jnp.bfloat16),
        in_specs=[hbm, hbm, hbm, hbm, vmem],
        out_specs=hbm,
        scratch_shapes=[
            pltpu.VMEM((rank_count, count, block, depth), jnp.bfloat16),
            pltpu.VMEM((pairs, count, block, cols), jnp.bfloat16),
            pltpu.VMEM((pairs * cols, rows), jnp.bfloat16),
            pltpu.VMEM((4, cols, depth), jnp.bfloat16),
            pltpu.VMEM((count, depth, cols), jnp.bfloat16),
            pltpu.VMEM((pairs * cols, rows), jnp.float32),
            dma((1,)),
            dma((pairs,)),
            dma((rank_count, count)),
            dma((rank_count,)),
            dma((zs, 2)),
            dma((zs,)),
            dma((pairs, 3)),
            dma((pairs, count)),
            dma((2,)),
            dma((3,)),
            dma((count,)),
        ],
        compiler_params=pltpu.CompilerParams(
            collective_id=0, has_side_effects=True, vmem_limit_bytes=62 * 1024 * 1024
        ),
        cost_estimate=pl.CostEstimate(
            flops=4 * pairs * points * rows * cols, bytes_accessed=4 * points * rows, transcendentals=0
        ),
    )(cols_pad, line, half, kernel, early)


CUTS = 7


def tail_kernel(
    back_ref, turned, other_ref, rowen_ref, virt_ref, res_ref, sq_ref,
    part, msend, mrecv, zsend, outer, inner, fin, oth, sq, sqall,
    ms, mr, zs_sem, outr, inr, fs, fr, osem, rsem, qs, qr,
):
    v = lax.axis_index("vpair")
    r = lax.axis_index("rank")
    y, x = v // 2, v % 2
    z, core = r // 2, r % 2
    near = (y * 2 + 1 - x, (1 - y) * 2 + x, (1 - y) * 2 + 1 - x)
    mate = z * 2 + 1 - core
    pairs, count, block, cols = back_ref.shape
    rows = part.shape[1]
    turns = pairs // 2
    step_rows = -(-rows // (16 * CUTS)) * 16
    cuts = [(h * step_rows, min(step_rows, rows - h * step_rows)) for h in range(CUTS)]
    at_end = jnp.logical_or(z == 0, z == 3)
    in_middle = jnp.logical_not(at_end)
    toward_at = (v, jnp.where(z < 2, z + 1, z - 1) * 2 + core)
    away_at = (v, jnp.where(z == 1, 0, 3) * 2 + core)
    mate_at = (v, mate)

    barrier = pltpu.get_barrier_semaphore()
    for peer in [(at, r) for at in near] + [mate_at, toward_at]:
        pl.semaphore_signal(barrier, inc=1, device_id=peer, device_id_type=MESH_IDS)

    @pl.when(in_middle)
    def _():
        pl.semaphore_signal(barrier, inc=1, device_id=away_at, device_id_type=MESH_IDS)
        pl.semaphore_wait(barrier, 6)

    @pl.when(at_end)
    def _():
        pl.semaphore_wait(barrier, 5)

    def remote(src, dst, send_sem, recv_sem, to):
        return pltpu.make_async_remote_copy(
            src_ref=src, dst_ref=dst, send_sem=send_sem, recv_sem=recv_sem,
            device_id=to, device_id_type=MESH_IDS,
        )

    def arrive(ref, sem):
        pltpu.make_async_copy(ref, ref, sem).wait()

    def other_copy(p):
        return pltpu.make_async_copy(other_ref.at[:, p], oth.at[p], osem.at[p])

    def cut(ref, t, h):
        return ref.at[t, pl.ds(*cuts[h]), :]

    def read(ref, t, h):
        return ref[t, pl.ds(*cuts[h]), :].astype(jnp.float32)

    def res_copy(p, h):
        return pltpu.make_async_copy(cut(oth, p, h), res_ref.at[pl.ds(*cuts[h]), p], rsem.at[p, h])

    def mate_copy(t):
        return remote(msend.at[t], mrecv.at[t], ms.at[t], mr.at[t], mate_at)

    def outer_copy(t, h):
        return remote(cut(zsend, t, h), cut(outer, t, h), zs_sem.at[t, h], outr.at[t, h], toward_at)

    def inner_copy(t, h):
        return remote(cut(zsend, t, h), cut(inner, t, h), zs_sem.at[t, h], inr.at[t, h], toward_at)

    def fin_copy(p, h, j, to):
        return remote(cut(fin, p, h), cut(fin, p, h), fs.at[p // 2, h, j], fr.at[p, h], to)

    def ladder(p):
        left = jnp.concatenate([back_ref[p, j] for j in range(count)], axis=1)
        return jnp.dot(left, turned[...], preferred_element_type=jnp.float32)[:rows]

    def make(t):
        msend[t] = ladder(2 * t + 1 - core).astype(jnp.bfloat16)
        mate_copy(t).start()
        part[t] = ladder(2 * t + core)

    def give(t, h):
        if h == 0:
            arrive(mrecv.at[t], mr.at[t])

        @pl.when(at_end)
        def _():
            zsend[t, pl.ds(*cuts[h]), :] = (read(part, t, h) + read(mrecv, t, h)).astype(jnp.bfloat16)
            outer_copy(t, h).start()

    def meet(t, h):
        @pl.when(in_middle)
        def _():
            arrive(cut(outer, t, h), outr.at[t, h])
            both = read(part, t, h) + read(mrecv, t, h)
            zsend[t, pl.ds(*cuts[h]), :] = (both + read(outer, t, h)).astype(jnp.bfloat16)
            inner_copy(t, h).start()

    def close(t, h):
        p = 2 * t + core

        @pl.when(in_middle)
        def _():
            arrive(cut(inner, t, h), inr.at[t, h])
            fin[p, pl.ds(*cuts[h]), :] = (read(zsend, t, h) + read(inner, t, h)).astype(jnp.bfloat16)
            fin_copy(p, h, 0, away_at).start()
            fin_copy(p, h, 1, mate_at).start()

    def land(t, h):
        p = 2 * t + core

        @pl.when(at_end)
        def _():
            arrive(cut(fin, p, h), fr.at[p, h])
            fin_copy(p, h, 1, mate_at).start()

    def settle(t, h):
        q = 2 * t + 1 - core
        arrive(cut(fin, q, h), fr.at[q, h])
        for e in range(2):
            p = 2 * t + e
            if h == 0:
                other_copy(p).wait()
            value = read(oth, p, h) + read(fin, p, h)
            oth[p, pl.ds(*cuts[h]), :] = value
            update = value / (rowen_ref[p, pl.ds(*cuts[h]), :] + virt_ref[...])
            squares = jnp.sum(update * update, axis=0, keepdims=True)
            if h == 0:
                sq[pl.ds(p, 1), :] = squares
            else:
                sq[pl.ds(p, 1), :] += squares
            res_copy(p, h).start()

    @pl.loop(0, pairs)
    def _(p):
        other_copy(p).start()

    stages = ((1, give), (3, meet), (5, close), (7, land), (9, settle))
    last = stages[-1][0]

    @pl.loop(0, turns + -(-last // CUTS))
    def _(u):
        @pl.when(u < turns)
        def _():
            make(u)

        for h in range(CUTS):
            for lag, stage in stages:
                t = u + (h - lag) // CUTS

                @pl.when(jnp.logical_and(t >= 0, t < turns))
                def _():
                    stage(t, (h - lag) % CUTS)

    sqall[v] = sq[...]
    for j in range(3):
        remote(sq, sqall.at[v], qs.at[j], qr.at[v], (near[j], r)).start()
    for at in near:
        arrive(sqall.at[at], qr.at[at])
    total = (sqall[0] + sqall[1]) + (sqall[2] + sqall[3])
    sq_ref[...] = jnp.sum(jnp.sum(total, axis=1, keepdims=True), axis=0, keepdims=True)

    for j in range(3):
        remote(sq, sqall.at[v], qs.at[j], qr.at[v], (near[j], r)).wait_send()

    @pl.loop(0, turns)
    def _(t):
        mate_copy(t).wait_send()
        for h in range(CUTS):
            outer_copy(t, h).wait_send()
            fin_copy(2 * t + core, h, 1, mate_at).wait_send()

            @pl.when(in_middle)
            def _():
                fin_copy(2 * t + core, h, 0, away_at).wait_send()

            for e in range(2):
                res_copy(2 * t + e, h).wait()


def ladder_tail(back, turned, other_turned, row_energy, virt_energy):
    pairs, count, block, cols = back.shape
    rows = other_turned.shape[0]
    depth, virt_count = turned.shape
    turns = pairs // 2
    hbm = pl.BlockSpec(memory_space=pl.ANY)
    vmem = pl.BlockSpec(memory_space=pltpu.VMEM)
    dma = pltpu.SemaphoreType.DMA
    bf16 = lambda *shape: pltpu.VMEM(shape, jnp.bfloat16)
    f32 = lambda *shape: pltpu.VMEM(shape, jnp.float32)
    return pl.pallas_call(
        tail_kernel,
        out_shape=(
            jax.ShapeDtypeStruct((rows, pairs, virt_count), jnp.float32),
            jax.ShapeDtypeStruct((1, 1), jnp.float32),
        ),
        in_specs=[vmem, vmem, hbm, vmem, vmem],
        out_specs=(hbm, vmem),
        scratch_shapes=[
            f32(turns, rows, virt_count),
            bf16(turns, rows, virt_count),
            bf16(turns, rows, virt_count),
            bf16(turns, rows, virt_count),
            bf16(turns, rows, virt_count),
            bf16(turns, rows, virt_count),
            bf16(pairs, rows, virt_count),
            f32(pairs, rows, virt_count),
            f32(pairs, virt_count),
            f32(count, pairs, virt_count),
            dma((turns,)),
            dma((turns,)),
            dma((turns, CUTS)),
            dma((turns, CUTS)),
            dma((turns, CUTS)),
            dma((turns, CUTS, 2)),
            dma((pairs, CUTS)),
            dma((pairs,)),
            dma((pairs, CUTS)),
            dma((3,)),
            dma((count,)),
        ],
        compiler_params=pltpu.CompilerParams(
            collective_id=2, has_side_effects=True, vmem_limit_bytes=62 * 1024 * 1024
        ),
        cost_estimate=pl.CostEstimate(
            flops=2 * pairs * rows * virt_count * depth, bytes_accessed=8 * pairs * rows * virt_count,
            transcendentals=0,
        ),
    )(back, turned, other_turned, row_energy, virt_energy)


def fast_shards(amplitudes, factors, kernel, other_terms, virt_energy, pair_energy):
    vpair_count = lax.axis_size("vpair")
    rank_count = lax.axis_size("rank")
    pair_count, row_block, _ = amplitudes.shape
    virt_count = row_block * vpair_count
    block = -(-row_block // 16) * 16
    tall = -(-row_block // 64) * 64
    col_block = amplitudes.shape[2]
    deep = -(-col_block // 16) * 16
    factors_pad = jnp.pad(factors, ((0, block - row_block), (0, 0)))
    amps_pad = jnp.pad(
        amplitudes.transpose(2, 0, 1), ((0, deep - col_block), (0, 0), (0, tall - row_block))
    ).reshape(deep, pair_count * tall)
    cols_pad, half, early, line, turned = front_gather(
        factors_pad, amps_pad, kernel, pair_count, col_block, vpair_count, rank_count
    )
    back = ladder_middle(cols_pad, line, half, kernel, early, rank_count)
    row_energy = lax.dynamic_slice_in_dim(
        virt_energy, lax.axis_index("vpair") * row_block, row_block, 0
    )
    shifted = row_energy[None, :, None] - pair_energy[:, None, None]
    residual, squares = ladder_tail(
        back, turned, other_terms.transpose(1, 0, 2), shifted, virt_energy[None, :]
    )
    update_rms = jnp.sqrt(squares[0, 0] / (pair_count * virt_count * virt_count) + epsilon)
    return (residual.transpose(1, 0, 2), update_rms)


def pick(amplitudes, factors, kernel, other_terms, virt_energy, pair_energy):
    vpair_count = lax.axis_size("vpair")
    rank_count = lax.axis_size("rank")
    fits = (
        vpair_count == 4
        and rank_count == 8
        and amplitudes.shape[0] == 8
        and amplitudes.shape[1] == 2 * amplitudes.shape[2]
        and kernel.shape[1] % (128 * vpair_count) == 0
    )
    body = fast_shards if fits else shards
    return body(amplitudes, factors, kernel, other_terms, virt_energy, pair_energy)


def solution(mesh):
    placed = (
        P(None, "vpair", "rank"),
        P("vpair", "rank"),
        P("vpair", "rank"),
        P(None, "vpair", None),
        P(),
        P(),
    )
    return jax.shard_map(
        pick, mesh=mesh, in_specs=placed, out_specs=(P(None, "vpair", None), P()), check_vma=False
    )
```
